256 devices in a mesh: dp: 32 (over x, z), mp: 8 (over y, core).
Axes of the slice: x: 4, y: 4, z: 8, core: 2. Of those that a mesh axis runs over, the one named last changes fastest.
Arguments:
- query_emb: bfloat16 [8192, 768], P('dp'), may hold values from -6 to 6
- positive_list: int32 [8192], replicated, may hold values from 0 to 32767
- centroids: float32 [32768, 768], P(('dp', 'mp')), may hold values from -0.6 to 0.6
- first_moment: float32 [32768, 768], P(('dp', 'mp')), may hold values from -3 to 3
- second_moment: float32 [32768, 768], P(('dp', 'mp')), may hold values from 0.05 to 2
Outputs:
- new_centroids: float32 [32768, 768], P(('dp', 'mp'))
- new_first: float32 [32768, 768], P(('dp', 'mp'))
- new_second: float32 [32768, 768], P(('dp', 'mp'))
- mean_loss: float32 [], replicated
The draws below stay inside these ranges and needn't reach their ends.
All inputs are finite; a program needn't handle non-finite values.
Results may differ from the reference program's by a relative error of at most 0.00097.
Values may be sent and summed in bfloat16 or wider, within the bound.
A program may use at most 64 MiB of HBM per device.

```python
import math
import jax
import jax.numpy as jnp
from jax import lax

D = 768
LISTS = 32768
ROWS = 8192


def centroid_rows(key):
    base_scale = 3.5 / math.sqrt(D)
    base = jnp.clip(base_scale * jax.random.normal(key, (LISTS, D), jnp.float32), -0.6, 0.6)
    signs = jnp.where(jax.random.normal(jax.random.fold_in(key, 3), (LISTS, D), jnp.float32) >= 0.0, base_scale, -base_scale)
    list_ids = jnp.arange(LISTS, dtype=jnp.int32)
    peaked = (list_ids % 1024 == 5)[:, None]
    return jnp.where(peaked, signs, base)


def draw_centroids(key, part):
    return centroid_rows(jax.random.fold_in(key, 11))


def draw_query_emb(key, part):
    base_scale = 3.5 / math.sqrt(D)
    aligned_size = min(6.0, 290.0 / (base_scale * D))
    table_full = centroid_rows(jax.random.fold_in(key, 11))
    noise_key = jax.random.fold_in(key, 12)
    background = jnp.clip(jax.random.normal(noise_key, (ROWS, D), jnp.float32), -6.0, 6.0)
    row_ids = jnp.arange(ROWS, dtype=jnp.int32)
    picked = (row_ids // 64 * 1024 + 5) % LISTS
    aligned = aligned_size * jnp.sign(table_full[picked])
    chosen = (row_ids % 64 == 0)[:, None]
    values = jnp.where(chosen, aligned, background)
    return values.astype(jnp.bfloat16)


def set_ends(array, stream_key, least, top_value):
    place = [jax.random.randint(jax.random.fold_in(stream_key, axis), (), 0, length) for axis, length in enumerate(array.shape)]
    widest = array.shape.index(max(array.shape))
    neighbour = place[:widest] + [(place[widest] + 1) % array.shape[widest]] + place[widest + 1:]
    return array.at[tuple(place)].set(least).at[tuple(neighbour)].set(top_value)


def block_levels(rng, extent, shards, smallest, high):
    level, own = 1.0, jax.random.fold_in(rng, 6)
    for axis_at, blocks in shards:
        heights = jnp.exp(jax.random.uniform(jax.random.fold_in(own, axis_at), (blocks,), jnp.float32, smallest / len(shards), high / len(shards)))
        level = level * jnp.repeat(heights, extent[axis_at] // blocks).reshape([-1 if axis == axis_at else 1 for axis in range(len(extent))])
    return level


def normal_values(own_key, extent, width, bound, cuts=(), kind=jnp.bfloat16):
    drawn = width * jax.random.normal(own_key, extent, jnp.float32)
    if cuts:
        drawn = drawn * block_levels(own_key, extent, cuts, -0.22, 0.18)
    return jnp.clip(drawn, -bound, bound).astype(kind)


def setup_inputs(seed: int = 0) -> dict:
    key_of = jax.random.split(jax.random.key(seed), 6)
    query_emb = draw_query_emb(jax.random.fold_in(key_of[5], 71), 0)
    positive_list = set_ends(jax.random.randint(key_of[1], (ROWS,), 0, LISTS), jax.random.fold_in(key_of[1], 1), 0, LISTS - 1).astype(jnp.int32)
    centroids = draw_centroids(jax.random.fold_in(key_of[5], 71), 0)
    first_moment = normal_values(key_of[3], (LISTS, D), 0.5, 3.0, ((0, 256),), jnp.float32)
    second_moment = jnp.clip(jnp.exp(math.log(2.0) - 3.6888794 * jax.random.uniform(key_of[4], (LISTS, D), jnp.float32) ** block_levels(key_of[4], (LISTS, D), ((0, 256),), -0.2, 0.2)), 0.05, 2.0)
    return {"query_emb": query_emb, "positive_list": positive_list, "centroids": centroids, "first_moment": first_moment, "second_moment": second_moment}


beta_first = 0.9
beta_second = 0.95
learn_rate = 0.01
epsilon = 1e-08

def adam_update(centroids, first_moment, second_moment, gradient):
    new_first = beta_first * first_moment + (1.0 - beta_first) * gradient
    new_second = beta_second * second_moment + (1.0 - beta_second) * gradient * gradient
    new_centroids = centroids - learn_rate * new_first / (jnp.sqrt(new_second) + epsilon)
    return (new_centroids, new_first, new_second)

def reference(query_emb, positive_list, centroids, first_moment, second_moment):
    table_half = centroids.astype(jnp.bfloat16)
    block_rows = math.gcd(ROWS, 512)
    query_blocks = query_emb.reshape(ROWS // block_rows, block_rows, D)
    target_blocks = positive_list.reshape(ROWS // block_rows, block_rows)
    list_ids = jnp.arange(LISTS, dtype=jnp.int32)

    def scan_step(state_pair, block_item):
        gradient, loss_sum = state_pair
        queries, targets = block_item
        logits = jnp.dot(queries, table_half.T, preferred_element_type=jnp.float32)
        row_peak = lax.optimization_barrier(jnp.max(logits, axis=1))
        row_mass = lax.optimization_barrier(jnp.sum(jnp.exp(logits - row_peak[:, None]), axis=1))
        log_norm = row_peak + jnp.log(row_mass)
        is_target = list_ids[None, :] == targets[:, None].astype(jnp.int32)
        row_target = lax.optimization_barrier(jnp.sum(jnp.where(is_target, logits, jnp.zeros_like(logits)), axis=1))
        loss_sum = loss_sum + jnp.sum(log_norm - row_target)
        weights = (jnp.exp(logits - log_norm[:, None]) - is_target.astype(jnp.float32)).astype(jnp.bfloat16)
        gradient = gradient + jnp.dot(weights.T, queries, preferred_element_type=jnp.float32)
        return ((gradient, loss_sum), None)
    start_state = (jnp.zeros((LISTS, D), jnp.float32), jnp.zeros((), jnp.float32))
    final_state, unused = lax.scan(scan_step, start_state, (query_blocks, target_blocks))
    gradient, loss_sum = final_state
    new_centroids, new_first, new_second = adam_update(centroids, first_moment, second_moment, gradient)
    return (new_centroids, new_first, new_second, loss_sum / ROWS)
```

```python
import jax
import jax.numpy as jnp
from jax import lax
from jax.experimental import pallas as pl
from jax.experimental.pallas import tpu as pltpu
from jax.sharding import Mesh
from jax.sharding import PartitionSpec as P

NX, NZ, NY, NC = 4, 8, 4, 2
AXES = ("x", "z", "y", "c")
DP = ("x", "z")
DP_MP = ("x", "z", "y", "c")
MESH = pl.DeviceIdType.MESH

ROWS = 8192
D = 768
LISTS = 32768
BLOCKS = NX * NZ
CLASSES = 4
BLOCK_ROWS = ROWS // BLOCKS // CLASSES
DEV_ROWS = BLOCKS * BLOCK_ROWS
OWN = LISTS // (NX * NZ * NY * NC)
HELD = 4 * OWN
TILES = DEV_ROWS // 128
GROUP = 4 * BLOCK_ROWS
SENDS = 31
PARTS = 4

beta_first = 0.9
beta_second = 0.95
learn_rate = 0.01
epsilon = 1e-08


def adam_update(centroids, first_moment, second_moment, gradient):
    new_first = beta_first * first_moment + (1.0 - beta_first) * gradient
    new_second = beta_second * second_moment + (1.0 - beta_second) * gradient * gradient
    new_centroids = centroids - learn_rate * new_first / (jnp.sqrt(new_second) + epsilon)
    return (new_centroids, new_first, new_second)


def log_sum_exp(slots):
    top = slots[0]
    for part in slots[1:]:
        top = jnp.maximum(top, part)
    total = jnp.exp(slots[0] - top)
    for part in slots[1:]:
        total = total + jnp.exp(part - top)
    return top + jnp.log(total)


def kernel(
    query_hbm, pos_ref, cent_ref, grad_ref, loss_ref,
    q, table, logits, weights, norm, stat1, stat2, loss1, loss2, loss3, part, from_partner, y_out, y_in,
    own_sem, q_send, q_recv, t_send, t_recv,
    s1_send, s1_recv, s2_send, s2_recv, l1_send, l1_recv, l2_send, l2_recv, l3_send, l3_recv,
    d_send, d_recv, y_send, y_recv,
):
    x, z, y, c = (lax.axis_index(a) for a in AXES)
    turn = 1 - 2 * c

    def at_x(k):
        return lax.rem(x + (k + NX), NX)

    def at_z(k):
        return lax.rem(z + (k + NZ), NZ)

    def at_y(k):
        return lax.rem(y + (k + NY), NY)

    helper_y = at_y(turn)
    owner_y = at_y(-turn)
    other = 1 - c

    def remote(src, dst, send, recv, where):
        copy = pltpu.make_async_remote_copy(
            src_ref=src, dst_ref=dst, send_sem=send, recv_sem=recv, device_id=where, device_id_type=MESH
        )
        copy.start()
        return copy

    def arrived(dst, sem):
        pltpu.make_async_copy(dst, dst, sem).wait()

    row_class = lax.rem(y, 2) * 2 + c
    own_place = jnp.where(c == 0, z * NX + x, x * NZ + z)
    own_copy = pltpu.make_async_copy(
        query_hbm.at[pl.ds(pl.multiple_of(row_class * BLOCK_ROWS, BLOCK_ROWS), BLOCK_ROWS)], q.at[own_place], own_sem
    )
    own_copy.start()
    table[0] = cent_ref[...].astype(jnp.bfloat16)

    group1 = [(dx, dy) for dy in (0, 2) for dx in range(NX) if (dx, dy) != (0, 0)]
    peers = [{"x": at_x(dx), "y": at_y(dy)} for dx, dy in group1]
    peers += [{"z": at_z(dz)} for dz in range(1, NZ)]
    peers += [{"y": at_y(1)}, {"y": at_y(-1)}, {"c": other}, {"y": helper_y, "c": other}]
    barrier = pltpu.get_barrier_semaphore()
    for peer in peers:
        pl.semaphore_signal(barrier, inc=1, device_id=peer, device_id_type=MESH)
    pl.semaphore_wait(barrier, len(peers))

    own_copy.wait()

    table_sends = [
        remote(table.at[0], table.at[1], t_send.at[0], t_recv.at[0], {"y": helper_y}),
        remote(table.at[0], table.at[2], t_send.at[1], t_recv.at[1], {"c": other}),
        remote(table.at[0], table.at[3], t_send.at[2], t_recv.at[2], {"y": helper_y, "c": other}),
    ]

    right, left = {"x": at_x(1)}, {"x": at_x(-1)}
    up, down = {"z": at_z(1)}, {"z": at_z(-1)}

    def passes(place_of):
        count = [0]

        def send(bx, bz, where):
            place = place_of(bx, bz)
            k = count[0]
            count[0] += 1
            remote(q.at[place], q.at[place], q_send.at[k], q_recv.at[place], where)

        def take(bx, bz):
            place = place_of(bx, bz)
            arrived(q.at[place], q_recv.at[place])

        return send, take, count

    send_a, take_a, count_a = passes(lambda bx, bz: bz * NX + bx)
    columns = (0, -1, 1, 2)

    def round_a(r):
        if r == 0:
            send_a(x, z, right)
            send_a(x, z, left)
            send_a(x, z, up)
            send_a(x, z, down)
            take_a(at_x(-1), z)
            send_a(at_x(-1), z, right)
            send_a(at_x(-1), z, up)
            send_a(at_x(-1), z, down)
            take_a(at_x(1), z)
            send_a(at_x(1), z, up)
            send_a(at_x(1), z, down)
            take_a(at_x(2), z)
            send_a(at_x(2), z, up)
            send_a(at_x(2), z, down)
        elif r in (1, 3, 5):
            s = (r + 1) // 2
            for j, k in enumerate(columns):
                bx = at_x(k)
                take_a(bx, at_z(-s))
                if s < 3 or j < 2:
                    send_a(bx, at_z(-s), up)
                take_a(bx, at_z(s))
                if s < 3 or j >= 2:
                    send_a(bx, at_z(s), down)
        elif r == 7:
            for k in columns:
                take_a(at_x(k), at_z(4))

    def place_a(r):
        s = (r + 1) // 2
        return at_z(-s if r % 2 else s) * GROUP

    send_b, take_b, count_b = passes(lambda bx, bz: bx * NZ + bz)
    along = (0, -1, 1, -2, 2, -3, 3, 4)

    def round_b(r):
        if r == 0:
            send_b(x, z, up)
            send_b(x, z, down)
            send_b(x, z, right)
            send_b(x, z, left)
            for k in along[1:]:
                take_b(x, at_z(k))
                if -4 < k < 0:
                    send_b(x, at_z(k), up)
                elif 0 < k < 3:
                    send_b(x, at_z(k), down)
                send_b(x, at_z(k), right)
                send_b(x, at_z(k), left)
        elif r == 2:
            for t, k in enumerate(along):
                take_b(at_x(-1), at_z(k))
                if t % 2 == 0:
                    send_b(at_x(-1), at_z(k), right)
                take_b(at_x(1), at_z(k))
                if t % 2 == 1:
                    send_b(at_x(1), at_z(k), left)
        elif r == 6:
            for k in along:
                take_b(at_x(2), at_z(k))

    def place_b(r):
        return at_x((0, -1, 1, 2)[r // 2]) * 2 * GROUP + (r % 2) * GROUP

    def move(r):
        @pl.when(c == 0)
        def _():
            round_a(r)

        @pl.when(c == 1)
        def _():
            round_b(r)

    def group_logits(r):
        start = pl.multiple_of(jnp.where(c == 0, place_a(r), place_b(r)), GROUP)
        rows = q[pl.ds(start // BLOCK_ROWS, 4)].reshape(GROUP, D)
        block = lax.dot_general(
            table[...].reshape(HELD, D), rows, (((1,), (1,)), ((), ())), preferred_element_type=jnp.float32
        )
        logits[:, pl.ds(start, GROUP)] = block
        peak = jnp.max(block, axis=0, keepdims=True)
        mass = jnp.sum(jnp.exp(block - peak), axis=0, keepdims=True)
        local = peak + jnp.log(mass)
        tile = start // 128
        norm[pl.ds(tile, 1), :] = local[:, :128]
        norm[pl.ds(tile + 1, 1), :] = local[:, 128:]

    move(0)
    move(1)
    for k in range(3):
        arrived(table.at[k + 1], t_recv.at[k])
    for r in range(8):
        group_logits(r)
        if r < 6:
            move(r + 2)
    assert count_a[0] == SENDS and count_b[0] == SENDS

    me1 = lax.div(y, 2) * NX + x

    def exchange1(slots, send, recv):
        for k, (dx, dy) in enumerate(group1):
            remote(slots.at[me1], slots.at[me1], send.at[k], recv.at[me1], {"x": at_x(dx), "y": at_y(dy)})

    def wait1(slots, send, recv):
        for k, (dx, dy) in enumerate(group1):
            place = lax.div(at_y(dy), 2) * NX + at_x(dx)
            arrived(slots.at[place], recv.at[place])
            arrived(slots.at[0], send.at[k])

    def exchange2(slots, send, recv):
        for dz in range(1, NZ):
            remote(slots.at[z], slots.at[z], send.at[dz - 1], recv.at[z], {"z": at_z(dz)})

    def wait2(slots, send, recv):
        for dz in range(1, NZ):
            arrived(slots.at[at_z(dz)], recv.at[at_z(dz)])
            arrived(slots.at[0], send.at[dz - 1])

    stat1[me1] = norm[...]
    exchange1(stat1, s1_send, s1_recv)
    wait1(stat1, s1_send, s1_recv)
    stat2[z] = log_sum_exp([stat1[k] for k in range(8)])
    exchange2(stat2, s2_send, s2_recv)
    wait2(stat2, s2_send, s2_recv)
    norm[...] = log_sum_exp([stat2[k] for k in range(8)])

    parity = lax.rem(y, 2)
    lane = lax.broadcasted_iota(jnp.int32, (1, 128), 1)
    sub = lax.broadcasted_iota(jnp.int32, (OWN, 128), 0)
    first_block = (x * NZ + z) * NY * NC
    held = [(y, c), (owner_y, c), (y, other), (helper_y, other)]
    ids = [sub + (first_block + hy * NC + hc) * OWN for hy, hc in held]

    def targets(b):
        return pos_ref[pl.ds(b * 2 + parity, 1), :]

    def tile_weights(j, loss):
        start = pl.multiple_of(j * 128, 128)
        even, odd = 2 * j, 2 * j + 1
        b0 = jnp.where(c == 0, lax.rem(even, NX) * NZ + lax.div(even, NX), even)
        b1 = jnp.where(c == 0, lax.rem(odd, NX) * NZ + lax.div(odd, NX), odd)
        r0, r1 = targets(b0), targets(b1)
        low = jnp.where(c == 0, r0, pltpu.roll(r0, 64, 1))
        high = jnp.where(c == 0, pltpu.roll(r1, 64, 1), r1)
        chosen = jnp.where(lane < 64, low, high)
        log_norm = norm[pl.ds(j, 1), :]
        for k in range(4):
            gap = logits[pl.ds(k * OWN, OWN), pl.ds(start, 128)] - log_norm
            is_target = ids[k] == chosen
            soft = jnp.exp(gap)
            weights[pl.ds(k * OWN, OWN), pl.ds(start, 128)] = jnp.where(is_target, soft - 1.0, soft).astype(
                jnp.bfloat16
            )
            missed = jnp.where(is_target, gap, 0.0)
            loss = loss - jnp.sum(missed.reshape(OWN // 8, 8, 128), axis=0)
        return loss

    loss = lax.fori_loop(0, TILES, tile_weights, jnp.zeros((8, 128), jnp.float32))
    loss1[me1] = loss
    exchange1(loss1, l1_send, l1_recv)

    def pair_gradient(first):
        def columns_of(n, carry):
            cols = pl.ds(pl.multiple_of(n * 256, 256), 256)
            part[pl.ds(first * OWN, 2 * OWN), cols] = jnp.dot(
                weights[pl.ds(first * OWN, 2 * OWN), :],
                q[:, :, cols].reshape(DEV_ROWS, 256),
                preferred_element_type=jnp.float32,
            )
            return carry

        lax.fori_loop(0, D // 256, columns_of, 0)

    pair_gradient(2)
    partner = {"c": other}
    to_partner = [
        remote(part.at[pl.ds(3 * OWN, OWN)], from_partner.at[1], d_send.at[1], d_recv.at[1], partner),
        remote(part.at[pl.ds(2 * OWN, OWN)], from_partner.at[0], d_send.at[0], d_recv.at[0], partner),
    ]
    pair_gradient(0)
    arrived(from_partner.at[1], d_recv.at[1])
    size = OWN // PARTS
    to_owner = []
    for k in range(PARTS):
        y_out[k] = part[pl.ds(OWN + k * size, size), :] + from_partner[1, pl.ds(k * size, size), :]
        to_owner.append(remote(y_out.at[k], y_in.at[k], y_send.at[k], y_recv.at[k], {"y": owner_y}))

    wait1(loss1, l1_send, l1_recv)
    total = loss1[0]
    for k in range(1, 8):
        total = total + loss1[k]
    loss2[z] = total
    exchange2(loss2, l2_send, l2_recv)

    arrived(from_partner.at[0], d_recv.at[0])
    grad_ref[...] = part[pl.ds(0, OWN), :] + from_partner[0]

    wait2(loss2, l2_send, l2_recv)
    total = loss2[0]
    for k in range(1, 8):
        total = total + loss2[k]
    loss3[0] = total
    across = remote(loss3.at[0], loss3.at[1], l3_send.at[0], l3_recv.at[0], partner)
    across.wait()
    loss3[2] = loss3[0] + loss3[1]
    last = remote(loss3.at[2], loss3.at[3], l3_send.at[1], l3_recv.at[1], {"y": owner_y})
    for k in range(PARTS):
        arrived(y_in.at[k], y_recv.at[k])
        rows = pl.ds(k * size, size)
        grad_ref[rows, :] = grad_ref[rows, :] + y_in[k]
    last.wait()
    loss_ref[...] = jnp.sum(loss3[2] + loss3[3], keepdims=True) * (1.0 / ROWS)

    for k in range(SENDS):
        arrived(q.at[0], q_send.at[k])
    for copy in table_sends + to_partner + to_owner:
        copy.wait_send()


def shards(query_emb, positive_list, centroids, first_moment, second_moment):
    f32, bf16, dma = jnp.float32, jnp.bfloat16, pltpu.SemaphoreType.DMA
    vmem = pl.BlockSpec(memory_space=pltpu.VMEM)
    gradient, loss = pl.pallas_call(
        kernel,
        name="step",
        out_shape=(jax.ShapeDtypeStruct((OWN, D), f32), jax.ShapeDtypeStruct((1, 1), f32)),
        in_specs=[pl.BlockSpec(memory_space=pl.ANY), vmem, vmem],
        out_specs=(vmem, vmem),
        scratch_shapes=[
            pltpu.VMEM((BLOCKS, BLOCK_ROWS, D), bf16),
            pltpu.VMEM((4, OWN, D), bf16),
            pltpu.VMEM((HELD, DEV_ROWS), f32),
            pltpu.VMEM((HELD, DEV_ROWS), bf16),
            pltpu.VMEM((TILES, 128), f32),
            pltpu.VMEM((8, TILES, 128), f32),
            pltpu.VMEM((8, TILES, 128), f32),
            pltpu.VMEM((8, 8, 128), f32),
            pltpu.VMEM((8, 8, 128), f32),
            pltpu.VMEM((4, 8, 128), f32),
            pltpu.VMEM((HELD, D), f32),
            pltpu.VMEM((2, OWN, D), f32),
            pltpu.VMEM((PARTS, OWN // PARTS, D), f32),
            pltpu.VMEM((PARTS, OWN // PARTS, D), f32),
            dma, dma((SENDS,)), dma((BLOCKS,)), dma((3,)), dma((3,)),
            dma((7,)), dma((8,)), dma((7,)), dma((8,)), dma((7,)), dma((8,)), dma((7,)), dma((8,)), dma((2,)), dma((2,)),
            dma((2,)), dma((2,)), dma((PARTS,)), dma((PARTS,)),
        ],
        compiler_params=pltpu.CompilerParams(
            collective_id=0, has_side_effects=True, vmem_limit_bytes=48 * 1024 * 1024
        ),
    )(query_emb, positive_list.reshape(ROWS // 128, 128), centroids)
    return (*adam_update(centroids, first_moment, second_moment, gradient), loss[0, 0])


def solution(mesh):
    split = Mesh(mesh.devices.reshape(NX, NZ, NY, NC), AXES)
    placed = (P(DP, None), P(), P(DP_MP, None), P(DP_MP, None), P(DP_MP, None))
    return jax.shard_map(
        shards,
        mesh=split,
        in_specs=placed,
        out_specs=(P(DP_MP, None), P(DP_MP, None), P(DP_MP, None), P()),
        check_vma=False,
    )
```

```python
import jax
import jax.numpy as jnp
from jax import lax
from jax.experimental import pallas as pl
from jax.experimental.pallas import tpu as pltpu
from jax.sharding import Mesh
from jax.sharding import PartitionSpec as P

NX, NZ, NY, NC = 4, 8, 4, 2
AXES = ("x", "z", "y", "c")
DP = ("x", "z")
DP_MP = ("x", "z", "y", "c")
MESH = pl.DeviceIdType.MESH

ROWS = 8192
D = 768
LISTS = 32768
BLOCKS = NX * NZ
CLASSES = 4
BLOCK_ROWS = ROWS // BLOCKS // CLASSES
DEV_ROWS = BLOCKS * BLOCK_ROWS
OWN = LISTS // (NX * NZ * NY * NC)
HELD = 4 * OWN
TILES = DEV_ROWS // 128
GROUP = 4 * BLOCK_ROWS
PIECES = 2
PIECE = BLOCK_ROWS // PIECES
SENDS = 31 * PIECES
PARTS = 6
WIDTH = D // PARTS

beta_first = 0.9
beta_second = 0.95
learn_rate = 0.01
epsilon = 1e-08


def adam_update(centroids, first_moment, second_moment, gradient):
    new_first = beta_first * first_moment + (1.0 - beta_first) * gradient
    new_second = beta_second * second_moment + (1.0 - beta_second) * gradient * gradient
    new_centroids = centroids - learn_rate * new_first / (jnp.sqrt(new_second) + epsilon)
    return (new_centroids, new_first, new_second)


def log_sum_exp(slots):
    top = slots[0]
    for part in slots[1:]:
        top = jnp.maximum(top, part)
    total = jnp.exp(slots[0] - top)
    for part in slots[1:]:
        total = total + jnp.exp(part - top)
    return top + jnp.log(total)


STARTS = [('UDLR', 'dRuDLUr'), ('UDRL', 'UdDLR')]
CUTS = ((17, 41, 45, 55, 59, 62, 62, 62), (21, 32, 44, 56, 60, 62, 62, 62))
GROUPS = ((0, 1, -1, -2, 2, -3, 3, 4), (0, 1, -1, -2, 2, -3, 3, 4))
ROUTES = (
    (
        (-1, 0, 0, ""), (1, 0, 0, "L"), (0, -1, 0, "URL"), (0, 1, 0, "DLR"), (-1, 0, 1, "UD"), (1, 0, 1, "U"),
        (0, -2, 1, "U"), (0, -1, 1, ""), (0, 2, 1, "LRD"), (0, 1, 1, "L"), (2, 0, 1, ""), (2, 0, 0, "U"),
        (-1, -1, 0, ""), (0, -2, 0, "rRLU"), (1, -1, 0, ""), (0, 2, 0, "DR"), (-1, 1, 0, ""), (-1, -1, 1, "RU"),
        (1, 1, 0, "DL"), (-1, 1, 1, ""), (1, -1, 1, "U"), (1, 2, 1, "D"), (-1, 2, 1, "D"), (0, 3, 1, ""),
        (0, -3, 1, "LRU"), (1, 1, 1, "L"), (2, -1, 0, ""), (0, 3, 0, "DLR"), (1, -2, 0, "U"), (0, -3, 0, ""),
        (1, 2, 0, "L"), (2, -2, 0, "U"), (2, 1, 0, ""), (-1, -2, 0, "U"), (-1, -2, 1, ""), (1, 3, 1, "DL"),
        (1, -3, 1, "L"), (-1, 2, 0, ""), (1, -2, 1, ""), (-1, 3, 1, "D"), (2, 1, 1, "D"), (2, -1, 1, "U"),
        (0, 4, 1, ""), (0, 4, 0, "R"), (1, 3, 0, "DL"), (1, -3, 0, ""), (-1, -3, 1, ""), (2, -3, 0, "U"),
        (2, 2, 0, ""), (1, 4, 1, "L"), (-1, -3, 0, ""), (-1, 3, 0, ""), (2, 3, 1, ""), (-1, 4, 1, ""),
        (2, -2, 1, ""), (2, 2, 1, ""), (2, -3, 1, ""), (-1, 4, 0, ""), (1, 4, 0, ""), (2, 3, 0, ""), (2, 4, 0, ""),
        (2, 4, 1, ""),
    ),
    (
        (-1, 0, 0, "R"), (1, 0, 0, ""), (0, -1, 0, "ULR"), (0, 1, 0, "DLR"), (-1, 0, 1, "R"), (1, 0, 1, "DU"),
        (0, -1, 1, "UR"), (1, -1, 0, "L"), (0, 2, 1, "D"), (2, 0, 0, "D"), (0, -2, 0, "LUR"), (0, 1, 1, "R"),
        (1, 1, 0, "D"), (-1, -1, 0, ""), (1, -1, 1, ""), (0, 2, 0, "DR"), (-1, 1, 0, ""), (0, -2, 1, "UL"),
        (2, -1, 0, ""), (1, 1, 1, "DL"), (2, 0, 1, ""), (0, -3, 0, "R"), (1, -2, 0, "UL"), (0, 3, 1, "L"),
        (-1, -1, 1, "RU"), (2, 1, 0, ""), (1, -2, 1, "U"), (0, -3, 1, "RU"), (-1, -2, 0, ""), (1, 2, 0, ""),
        (2, 1, 1, ""), (-1, 1, 1, "D"), (1, -3, 0, "L"), (0, 3, 0, "RDL"), (2, -2, 0, ""), (-1, 2, 0, "R"),
        (-1, -2, 1, ""), (1, 2, 1, ""), (1, 3, 1, "LD"), (-1, -3, 0, ""), (1, -3, 1, ""), (-1, 2, 1, "DR"),
        (2, -3, 0, "U"), (2, -1, 1, "U"), (0, 4, 1, ""), (0, 4, 0, "L"), (1, 3, 0, ""), (-1, -3, 1, "UR"),
        (1, 4, 1, ""), (-1, 3, 0, "DR"), (2, 3, 1, "D"), (2, 4, 0, ""), (2, 2, 0, ""), (-1, 3, 1, ""), (1, 4, 0, ""),
        (2, -2, 1, ""), (2, 2, 1, ""), (2, -3, 1, ""), (-1, 4, 1, ""), (-1, 4, 0, ""), (2, 3, 0, ""), (2, 4, 1, ""),
    ),
)


def kernel(
    query_hbm, pos_hbm, cent_hbm, grad_ref, loss_ref,
    q, pos, cent, chosen, table, logits, weights, norm, hit, stat1, stat2, hit1, loss2, loss,
    part, from_partner, y_out, y_in,
    own_sem, q_send, q_recv, t_send, t_recv,
    s1_send, s1_recv, s2_send, s2_recv, h1_send, h1_recv, h2_send, h2_recv, l_send, l_recv,
    d_send, d_recv, y_send, y_recv,
):
    x, z, y, c = (lax.axis_index(a) for a in AXES)
    turn = 1 - 2 * c

    def at_x(k):
        return lax.rem(x + (k + NX), NX)

    def at_z(k):
        return lax.rem(z + (k + NZ), NZ)

    def at_y(k):
        return lax.rem(y + (k + NY), NY)

    helper_y = at_y(turn)
    owner_y = at_y(-turn)
    other = 1 - c
    partner = {"c": other}

    group1 = [(dx, dy) for dy in (0, 2) for dx in range(NX) if (dx, dy) != (0, 0)]
    peers = [{"x": at_x(dx)} for dx in (1, -1, 2)]
    peers += [{"z": at_z(dz)} for dz in (1, -1, 2, -2)]
    peers += [{"y": at_y(1)}, {"y": at_y(-1)}, partner, {"y": helper_y, "c": other}]
    barrier = pltpu.get_barrier_semaphore()
    for peer in peers:
        pl.semaphore_signal(barrier, inc=1, device_id=peer, device_id_type=MESH)

    def remote(src, dst, send, recv, where):
        copy = pltpu.make_async_remote_copy(
            src_ref=src, dst_ref=dst, send_sem=send, recv_sem=recv, device_id=where, device_id_type=MESH
        )
        copy.start()
        return copy

    def arrived(dst, sem):
        pltpu.make_async_copy(dst, dst, sem).wait()

    row_class = lax.rem(y, 2) * 2 + c
    own_place = z * NX + x
    local = [
        pltpu.make_async_copy(
            query_hbm.at[pl.ds(pl.multiple_of(row_class * BLOCK_ROWS + p * PIECE, PIECE), PIECE)],
            q.at[own_place, p],
            own_sem.at[p],
        )
        for p in range(PIECES)
    ]
    local.append(pltpu.make_async_copy(cent_hbm, cent, own_sem.at[PIECES]))
    local.append(pltpu.make_async_copy(pos_hbm, pos, own_sem.at[PIECES + 1]))
    for copy in local:
        copy.start()
    for copy in local:
        copy.wait()
    table[0] = cent[...].astype(jnp.bfloat16)
    pl.semaphore_wait(barrier, len(peers))

    toward = {"R": {"x": at_x(1)}, "L": {"x": at_x(-1)}, "U": {"z": at_z(1)}, "D": {"z": at_z(-1)}}
    toward |= {"r": {"x": at_x(2)}, "l": {"x": at_x(2)}, "u": {"z": at_z(2)}, "d": {"z": at_z(-2)}}

    def carrier():
        count = [0]

        def send(dx, dz, p, links):
            place = at_z(dz) * NX + at_x(dx)
            for link in links:
                remote(
                    q.at[place, p], q.at[place, p], q_send.at[count[0]], q_recv.at[place * PIECES + p], toward[link]
                )
                count[0] += 1

        return send, count

    carriers = [carrier() for _ in range(NC)]

    def move(r):
        for core in range(NC):
            send, _ = carriers[core]
            cuts = (0, *CUTS[core])
            events = ROUTES[core][cuts[r] : cuts[r + 1]]

            @pl.when(c == core)
            def _(send=send, core=core, events=events):
                if r == 0:
                    for p in range(PIECES):
                        send(0, 0, p, STARTS[core][p])
                for dx, dz, p, links in events:
                    place = at_z(dz) * NX + at_x(dx)
                    arrived(q.at[place, p], q_recv.at[place * PIECES + p])
                    send(dx, dz, p, links)

    parity = lax.rem(y, 2)
    lane = lax.broadcasted_iota(jnp.int32, (1, 128), 1)

    def targets(bz, bx):
        return pos[pl.ds((bx * NZ + bz) * 2 + parity, 1), :]

    def choose():
        for j in range(TILES):
            r0, r1 = targets(j // 2, 2 * (j % 2)), targets(j // 2, 2 * (j % 2) + 1)
            low = jnp.where(c == 0, r0, pltpu.roll(r0, 64, 1))
            high = jnp.where(c == 0, pltpu.roll(r1, 64, 1), r1)
            chosen[j : j + 1, :] = jnp.where(lane < 64, low, high)

    sub = lax.broadcasted_iota(jnp.int32, (OWN, 128), 0)
    first_block = (x * NZ + z) * NY * NC
    held = [(y, c), (y, other), (owner_y, c), (helper_y, other)]
    firsts = [(first_block + hy * NC + hc) * OWN for hy, hc in held]

    def group_logits(r):
        group = jnp.where(c == 0, at_z(GROUPS[0][r]), at_z(GROUPS[1][r]))
        start = pl.multiple_of(group * GROUP, GROUP)
        rows = q[pl.ds(group * NX, NX)].reshape(GROUP, D)
        block = lax.dot_general(
            table[...].reshape(HELD, D), rows, (((1,), (1,)), ((), ())), preferred_element_type=jnp.float32
        )
        logits[:, pl.ds(start, GROUP)] = block
        peak = jnp.max(block, axis=0, keepdims=True)
        mass = jnp.sum(jnp.exp(block - peak), axis=0, keepdims=True)
        local_norm = peak + jnp.log(mass)
        for h in range(2):
            tile = group * 2 + h
            norm[pl.ds(tile, 1), :] = local_norm[:, h * 128 : h * 128 + 128]
            ids = chosen[pl.ds(tile, 1), :]
            found = jnp.zeros((1, 128), jnp.float32)
            for k in range(4):
                values = block[k * OWN : (k + 1) * OWN, h * 128 : h * 128 + 128]
                found = found + jnp.sum(jnp.where(sub + firsts[k] == ids, values, 0.0), axis=0, keepdims=True)
            hit[pl.ds(tile, 1), :] = found

    table_sends = [
        remote(table.at[0], table.at[1], t_send.at[0], t_recv.at[0], partner),
        remote(table.at[0], table.at[2], t_send.at[1], t_recv.at[1], {"y": helper_y}),
        remote(table.at[0], table.at[3], t_send.at[2], t_recv.at[2], {"y": helper_y, "c": other}),
    ]
    for r in range(8):
        move(r)
        if r == 0:
            choose()
            for k in range(3):
                arrived(table.at[k + 1], t_recv.at[k])
        group_logits(r)
    for _, count in carriers:
        assert count[0] == SENDS

    me1 = lax.div(y, 2) * NX + x

    def exchange1(slots, send, recv):
        for k, (dx, dy) in enumerate(group1):
            remote(slots.at[me1], slots.at[me1], send.at[k], recv.at[me1], {"x": at_x(dx), "y": at_y(dy)})

    def wait1(slots, send, recv):
        for k, (dx, dy) in enumerate(group1):
            place = lax.div(at_y(dy), 2) * NX + at_x(dx)
            arrived(slots.at[place], recv.at[place])
            arrived(slots.at[0], send.at[k])

    def exchange2(slots, send, recv):
        for dz in range(1, NZ):
            remote(slots.at[z], slots.at[z], send.at[dz - 1], recv.at[z], {"z": at_z(dz)})

    def wait2(slots, send, recv):
        for dz in range(1, NZ):
            arrived(slots.at[at_z(dz)], recv.at[at_z(dz)])
            arrived(slots.at[0], send.at[dz - 1])

    def summed(slots):
        total = slots[0]
        for k in range(1, 8):
            total = total + slots[k]
        return total

    stat1[me1] = norm[...]
    exchange1(stat1, s1_send, s1_recv)
    hit1[me1] = hit[...]
    exchange1(hit1, h1_send, h1_recv)
    wait1(stat1, s1_send, s1_recv)
    stat2[z] = log_sum_exp([stat1[k] for k in range(8)])
    exchange2(stat2, s2_send, s2_recv)
    wait2(stat2, s2_send, s2_recv)
    norm[...] = log_sum_exp([stat2[k] for k in range(8)])

    wait1(hit1, h1_send, h1_recv)
    here = lax.rem(lax.div(chosen[...], OWN * NY * NC), NZ) == z
    missed = jnp.where(here, norm[...] - summed(hit1), 0.0)
    loss2[z] = missed[:8] + missed[8:]
    exchange2(loss2, h2_send, h2_recv)

    def tile_weights(j, carry):
        start = pl.multiple_of(j * 128, 128)
        log_norm = norm[pl.ds(j, 1), :]
        ids = chosen[pl.ds(j, 1), :]
        for k in (2, 3, 0, 1):
            soft = jnp.exp(logits[pl.ds(k * OWN, OWN), pl.ds(start, 128)] - log_norm)
            soft = jnp.where(sub + firsts[k] == ids, soft - 1.0, soft)
            weights[pl.ds(k * OWN, OWN), pl.ds(start, 128)] = soft.astype(jnp.bfloat16)
        return carry

    lax.fori_loop(0, TILES, tile_weights, 0)

    def pair_gradient(first, n):
        part[n, first * OWN : (first + 2) * OWN, :] = jnp.dot(
            weights[first * OWN : (first + 2) * OWN, :],
            q[:, :, :, n * WIDTH : (n + 1) * WIDTH].reshape(DEV_ROWS, WIDTH),
            preferred_element_type=jnp.float32,
        )

    to_partner, to_owner = [], []

    def hand_over(n, slot):
        lists = part.at[n, pl.ds((1 + 2 * slot) * OWN, OWN)]
        to_partner.append(remote(lists, from_partner.at[n, slot], d_send.at[n, slot], d_recv.at[n, slot], partner))

    def give_back(n):
        arrived(from_partner.at[n, 1], d_recv.at[n, 1])
        y_out[n] = part[n, 2 * OWN : 3 * OWN, :] + from_partner[n, 1]
        to_owner.append(remote(y_out.at[n], y_in.at[n], y_send.at[n], y_recv.at[n], {"y": owner_y}))

    for n in range(PARTS):
        pair_gradient(2, n)
        hand_over(n, 1)
        if n:
            give_back(n - 1)
    give_back(PARTS - 1)
    wait2(loss2, h2_send, h2_recv)
    loss[0] = summed(loss2)
    loss_across = remote(loss.at[0], loss.at[1], l_send.at[0], l_recv.at[0], partner)
    for n in range(PARTS):
        pair_gradient(0, n)
        hand_over(n, 0)
    loss_across.wait()
    loss[2] = loss[0] + loss[1]
    loss_back = remote(loss.at[2], loss.at[3], l_send.at[1], l_recv.at[1], {"y": owner_y})
    for n in range(PARTS):
        arrived(from_partner.at[n, 0], d_recv.at[n, 0])
        arrived(y_in.at[n], y_recv.at[n])
        grad_ref[:, n * WIDTH : (n + 1) * WIDTH] = part[n, :OWN, :] + from_partner[n, 0] + y_in[n]
    loss_back.wait()
    loss_ref[...] = jnp.sum(loss[2] + loss[3], keepdims=True) * (1.0 / ROWS)

    for k in range(SENDS):
        arrived(q.at[0, 0], q_send.at[k])
    for copy in table_sends + to_partner + to_owner:
        copy.wait_send()


def shards(query_emb, positive_list, centroids, first_moment, second_moment):
    f32, bf16, i32, dma = jnp.float32, jnp.bfloat16, jnp.int32, pltpu.SemaphoreType.DMA
    vmem, hbm = pl.BlockSpec(memory_space=pltpu.VMEM), pl.BlockSpec(memory_space=pl.ANY)
    gradient, loss = pl.pallas_call(
        kernel,
        name="step",
        out_shape=(jax.ShapeDtypeStruct((OWN, D), f32), jax.ShapeDtypeStruct((1, 1), f32)),
        in_specs=[hbm, hbm, hbm],
        out_specs=(vmem, vmem),
        scratch_shapes=[
            pltpu.VMEM((BLOCKS, PIECES, PIECE, D), bf16),
            pltpu.VMEM((ROWS // 128, 128), i32),
            pltpu.VMEM((OWN, D), f32),
            pltpu.VMEM((TILES, 128), i32),
            pltpu.VMEM((4, OWN, D), bf16),
            pltpu.VMEM((HELD, DEV_ROWS), f32),
            pltpu.VMEM((HELD, DEV_ROWS), bf16),
            pltpu.VMEM((TILES, 128), f32),
            pltpu.VMEM((TILES, 128), f32),
            pltpu.VMEM((8, TILES, 128), f32),
            pltpu.VMEM((8, TILES, 128), f32),
            pltpu.VMEM((8, TILES, 128), f32),
            pltpu.VMEM((8, 8, 128), f32),
            pltpu.VMEM((4, 8, 128), f32),
            pltpu.VMEM((PARTS, HELD, WIDTH), f32),
            pltpu.VMEM((PARTS, 2, OWN, WIDTH), f32),
            pltpu.VMEM((PARTS, OWN, WIDTH), f32),
            pltpu.VMEM((PARTS, OWN, WIDTH), f32),
            dma((PIECES + 2,)), dma((SENDS,)), dma((BLOCKS * PIECES,)), dma((3,)), dma((3,)),
            dma((7,)), dma((8,)), dma((7,)), dma((8,)), dma((7,)), dma((8,)), dma((7,)), dma((8,)), dma((2,)), dma((2,)),
            dma((PARTS, 2)), dma((PARTS, 2)), dma((PARTS,)), dma((PARTS,)),
        ],
        compiler_params=pltpu.CompilerParams(collective_id=0, has_side_effects=True, vmem_limit_bytes=56000000),
    )(query_emb, positive_list.reshape(ROWS // 128, 128), centroids)
    return (*adam_update(centroids, first_moment, second_moment, gradient), loss[0, 0])


def solution(mesh):
    split = Mesh(mesh.devices.reshape(NX, NZ, NY, NC), AXES)
    placed = (P(DP, None), P(), P(DP_MP, None), P(DP_MP, None), P(DP_MP, None))
    return jax.shard_map(
        shards,
        mesh=split,
        in_specs=placed,
        out_specs=(P(DP_MP, None), P(DP_MP, None), P(DP_MP, None), P()),
        check_vma=False,
    )
```

```python
import jax
import jax.numpy as jnp
from jax import lax
from jax.experimental import pallas as pl
from jax.experimental.pallas import tpu as pltpu
from jax.sharding import Mesh
from jax.sharding import PartitionSpec as P

NX, NZ, NY, NC = 4, 8, 4, 2
AXES = ("x", "z", "y", "c")
DP = ("x", "z")
DP_MP = ("x", "z", "y", "c")
MESH = pl.DeviceIdType.MESH

ROWS = 8192
D = 768
LISTS = 32768
BLOCKS = NX * NZ
CLASSES = 4
BLOCK_ROWS = ROWS // BLOCKS // CLASSES
DEV_ROWS = BLOCKS * BLOCK_ROWS
OWN = LISTS // (NX * NZ * NY * NC)
HELD = 4 * OWN
TILES = DEV_ROWS // 128
GROUP = 4 * BLOCK_ROWS
PIECES = 2
PIECE = BLOCK_ROWS // PIECES
SENDS = 31 * PIECES
HALF = OWN // 2
PARTS = 3
WIDTH = D // PARTS

beta_first = 0.9
beta_second = 0.95
learn_rate = 0.01
epsilon = 1e-08


def adam_update(centroids, first_moment, second_moment, gradient):
    new_first = beta_first * first_moment + (1.0 - beta_first) * gradient
    new_second = beta_second * second_moment + (1.0 - beta_second) * gradient * gradient
    new_centroids = centroids - learn_rate * new_first / (jnp.sqrt(new_second) + epsilon)
    return (new_centroids, new_first, new_second)


def log_sum_exp(slots):
    top = slots[0]
    for part in slots[1:]:
        top = jnp.maximum(top, part)
    total = jnp.exp(slots[0] - top)
    for part in slots[1:]:
        total = total + jnp.exp(part - top)
    return top + jnp.log(total)


STARTS = [('DURL', 'udLrRDU'), ('URDL', 'UDLR')]
CUTS = ((16, 33, 41, 46, 51, 57, 61, 62), (20, 35, 39, 43, 47, 57, 61, 62))
GROUPS = ((0, 1, -1, 2, -2, -3, 3, 4), (0, 1, -2, -1, 2, -3, 3, 4))
ROUTES = (
    (
        (-1, 0, 0, "R"), (1, 0, 0, ""), (0, -1, 0, "uURL"), (0, 1, 0, "DRL"), (1, 0, 1, "U"), (2, 0, 1, "D"),
        (0, -2, 1, "UrR"), (0, 2, 1, "LRD"), (-1, 0, 1, "UD"), (0, -1, 1, ""), (0, 1, 1, "L"), (2, 0, 0, "D"),
        (1, -1, 0, ""), (0, 2, 0, "LDR"), (-1, -1, 0, "R"), (1, 1, 0, ""), (0, -3, 0, "RUL"), (-1, 1, 0, ""),
        (0, -2, 0, "LR"), (1, 2, 1, "D"), (2, 1, 1, "D"), (1, -1, 1, "UL"), (1, 1, 1, ""), (0, 3, 1, ""),
        (0, -3, 1, "UR"), (2, -2, 1, "U"), (-1, -2, 1, ""), (1, 2, 0, "L"), (-1, 1, 1, ""), (-1, -1, 1, ""),
        (-1, 2, 1, "D"), (1, -3, 0, "U"), (2, 1, 0, ""), (0, 4, 0, "r"), (-1, 2, 0, ""), (2, -1, 0, ""),
        (1, -2, 0, "L"), (0, 3, 0, "RL"), (1, -2, 1, "U"), (-1, -3, 0, "UR"), (2, -1, 1, ""), (1, 3, 1, "DL"),
        (0, 4, 1, "R"), (-1, -2, 0, ""), (2, 2, 0, "D"), (2, 2, 1, ""), (2, -3, 1, "U"), (-1, -3, 1, ""),
        (-1, 3, 1, ""), (1, 4, 0, ""), (2, -2, 0, ""), (1, -3, 1, ""), (2, 4, 0, ""), (-1, 3, 0, ""), (1, 3, 0, ""),
        (1, 4, 1, ""), (2, -3, 0, ""), (-1, 4, 0, ""), (2, 3, 1, ""), (2, 3, 0, ""), (-1, 4, 1, ""), (2, 4, 1, ""),
    ),
    (
        (-1, 0, 0, "D"), (1, 0, 0, "L"), (0, -1, 0, "URL"), (0, 1, 0, "DL"), (-1, 0, 1, "D"), (1, 0, 1, "DL"),
        (0, -1, 1, "RUL"), (0, 1, 1, "D"), (2, 0, 0, "D"), (-1, -1, 0, "R"), (0, -2, 0, "UR"), (-1, 1, 0, "D"),
        (1, -1, 0, "U"), (0, 2, 0, "LD"), (-1, -1, 1, "U"), (0, -2, 1, "UL"), (-1, 1, 1, ""), (1, 1, 0, ""),
        (1, 1, 1, "DL"), (2, 0, 1, ""), (2, -1, 0, "U"), (0, -3, 0, "LU"), (0, 2, 1, "RD"), (1, -1, 1, "L"),
        (-1, -2, 0, "U"), (1, -2, 0, ""), (2, 1, 0, ""), (1, 2, 0, "DL"), (-1, -2, 1, "RU"), (-1, 2, 0, "D"),
        (1, -2, 1, ""), (0, -3, 1, "UL"), (-1, 2, 1, "DR"), (0, 3, 0, ""), (2, 1, 1, ""), (2, -2, 0, ""),
        (1, 2, 1, "D"), (1, -3, 0, "L"), (2, -2, 1, "u"), (0, 4, 0, "RL"), (0, 3, 1, ""), (2, -1, 1, ""),
        (-1, -3, 0, ""), (2, 2, 1, "D"), (1, 3, 0, ""), (2, 2, 0, ""), (-1, -3, 1, ""), (-1, 3, 0, "R"),
        (1, -3, 1, "L"), (-1, 3, 1, "D"), (-1, 4, 0, ""), (0, 4, 1, "L"), (2, -3, 0, "U"), (1, 3, 1, ""),
        (1, 4, 0, ""), (2, 3, 1, ""), (2, -3, 1, ""), (2, 3, 0, ""), (-1, 4, 1, ""), (2, 4, 1, ""), (1, 4, 1, ""),
        (2, 4, 0, ""),
    ),
)


def kernel(
    query_hbm, pos_hbm, cent_hbm, grad_ref, loss_ref,
    q, pos, cent, chosen, table, logits, weights, norm, hit, stat1, stat2, hit1, loss2, loss,
    part, from_partner, y_out, y_in,
    own_sem, q_send, q_recv, t_send, t_recv,
    s1_send, s1_recv, s2_send, s2_recv, h1_send, h1_recv, h2_send, h2_recv, l_send, l_recv,
    d_send, d_recv, y_send, y_recv,
):
    x, z, y, c = (lax.axis_index(a) for a in AXES)

    def at_x(k):
        return lax.rem(x + (k + NX), NX)

    def at_z(k):
        return lax.rem(z + (k + NZ), NZ)

    def at_y(k):
        return lax.rem(y + (k + NY), NY)

    other = 1 - c
    partner = {"c": other}

    group1 = [(dx, dy) for dy in (0, 2) for dx in range(NX) if (dx, dy) != (0, 0)]
    peers = [{"x": at_x(k)} for k in (1, -1, 2)] + [{"z": at_z(k)} for k in (1, -1, 2, -2)]
    peers += [partner] + [{"y": at_y(k), "c": core} for k in (1, -1) for core in (c, other)]
    barrier = pltpu.get_barrier_semaphore()
    for peer in peers:
        pl.semaphore_signal(barrier, inc=1, device_id=peer, device_id_type=MESH)

    def remote(src, dst, send, recv, where):
        copy = pltpu.make_async_remote_copy(
            src_ref=src, dst_ref=dst, send_sem=send, recv_sem=recv, device_id=where, device_id_type=MESH
        )
        copy.start()
        return copy

    def arrived(dst, sem):
        pltpu.make_async_copy(dst, dst, sem).wait()

    row_class = lax.rem(y, 2) * 2 + c
    own_place = z * NX + x
    local = [
        pltpu.make_async_copy(
            query_hbm.at[pl.ds(pl.multiple_of(row_class * BLOCK_ROWS + p * PIECE, PIECE), PIECE)],
            q.at[own_place, p],
            own_sem.at[p],
        )
        for p in range(PIECES)
    ]
    local.append(pltpu.make_async_copy(cent_hbm, cent, own_sem.at[PIECES]))
    local.append(pltpu.make_async_copy(pos_hbm, pos, own_sem.at[PIECES + 1]))
    for copy in local:
        copy.start()
    pl.semaphore_wait(barrier, len(peers))
    for copy in local[:PIECES]:
        copy.wait()

    toward = {"R": {"x": at_x(1)}, "L": {"x": at_x(-1)}, "U": {"z": at_z(1)}, "D": {"z": at_z(-1)}}
    toward |= {"r": {"x": at_x(2)}, "l": {"x": at_x(2)}, "u": {"z": at_z(2)}, "d": {"z": at_z(-2)}}

    def carrier():
        count = [0]

        def send(dx, dz, p, links):
            place = at_z(dz) * NX + at_x(dx)
            for link in links:
                remote(
                    q.at[place, p], q.at[place, p], q_send.at[count[0]], q_recv.at[place * PIECES + p], toward[link]
                )
                count[0] += 1

        return send, count

    carriers = [carrier() for _ in range(NC)]

    def move(r):
        for core in range(NC):
            send, _ = carriers[core]
            cuts = (0, *CUTS[core])
            events = ROUTES[core][cuts[r] : cuts[r + 1]]

            @pl.when(c == core)
            def _(send=send, core=core, events=events):
                for dx, dz, p, links in events:
                    place = at_z(dz) * NX + at_x(dx)
                    arrived(q.at[place, p], q_recv.at[place * PIECES + p])
                    send(dx, dz, p, links)

    parity = lax.rem(y, 2)
    lane = lax.broadcasted_iota(jnp.int32, (1, 128), 1)

    def targets(bz, bx):
        return pos[pl.ds((bx * NZ + bz) * 2 + parity, 1), :]

    def choose():
        for j in range(TILES):
            r0, r1 = targets(j // 2, 2 * (j % 2)), targets(j // 2, 2 * (j % 2) + 1)
            low = jnp.where(c == 0, r0, pltpu.roll(r0, 64, 1))
            high = jnp.where(c == 0, pltpu.roll(r1, 64, 1), r1)
            chosen[j : j + 1, :] = jnp.where(lane < 64, low, high)

    sub = lax.broadcasted_iota(jnp.int32, (OWN, 128), 0)
    first_block = (x * NZ + z) * NY * NC
    held = [(0, OWN, y, c, 0), (OWN, OWN, y, other, 0)]
    for place, core in ((2 * OWN, c), (3 * OWN, other)):
        held += [(place, HALF, at_y(-1), core, 0), (place + HALF, HALF, at_y(1), core, HALF)]
    parts = [(place, lists, (first_block + hy * NC + hc) * OWN + first) for place, lists, hy, hc, first in held]

    def group_logits(r):
        group = jnp.where(c == 0, at_z(GROUPS[0][r]), at_z(GROUPS[1][r]))
        start = pl.multiple_of(group * GROUP, GROUP)
        rows = q[pl.ds(group * NX, NX)].reshape(GROUP, D)
        block = lax.dot_general(
            table[...], rows, (((1,), (1,)), ((), ())), preferred_element_type=jnp.float32
        )
        logits[:, pl.ds(start, GROUP)] = block
        peak = jnp.max(block, axis=0, keepdims=True)
        mass = jnp.sum(jnp.exp(block - peak), axis=0, keepdims=True)
        local_norm = peak + jnp.log(mass)
        for h in range(2):
            tile = group * 2 + h
            norm[pl.ds(tile, 1), :] = local_norm[:, h * 128 : h * 128 + 128]
            ids = chosen[pl.ds(tile, 1), :]
            found = jnp.zeros((1, 128), jnp.float32)
            for place, lists, first in parts:
                values = block[place : place + lists, h * 128 : h * 128 + 128]
                found = found + jnp.sum(jnp.where(sub[:lists] == ids - first, values, 0.0), axis=0, keepdims=True)
            hit[pl.ds(tile, 1), :] = found

    table_sends = []
    table_routes = [
        (0, 2 * OWN, HALF, {"y": at_y(1)}),
        (1, 2 * OWN + HALF, HALF, {"y": at_y(-1)}),
        (0, 3 * OWN, HALF, {"y": at_y(1), "c": other}),
        (1, 3 * OWN + HALF, HALF, {"y": at_y(-1), "c": other}),
        (0, OWN, OWN, partner),
    ]

    def share_table():
        local[PIECES].wait()
        table[:OWN, :] = cent[...].astype(jnp.bfloat16)
        for k, (half, place, rows, where) in enumerate(table_routes):
            source, target = table.at[pl.ds(half * HALF, rows)], table.at[pl.ds(place, rows)]
            table_sends.append(remote(source, target, t_send.at[k], t_recv.at[k], where))

    for core in range(NC):
        send, _ = carriers[core]

        @pl.when(c == core)
        def _(send=send, core=core):
            for p in range(PIECES):
                send(0, 0, p, STARTS[core][p])

    share_table()
    local[PIECES + 1].wait()
    for r in range(8):
        move(r)
        if r == 0:
            choose()
            for k, (_, place, rows, _) in enumerate(table_routes):
                arrived(table.at[pl.ds(place, rows)], t_recv.at[k])
        group_logits(r)
    for _, count in carriers:
        assert count[0] == SENDS

    me1 = lax.div(y, 2) * NX + x

    def exchange1(slots, send, recv):
        for k, (dx, dy) in enumerate(group1):
            remote(slots.at[me1], slots.at[me1], send.at[k], recv.at[me1], {"x": at_x(dx), "y": at_y(dy)})

    def wait1(slots, send, recv):
        for k, (dx, dy) in enumerate(group1):
            place = lax.div(at_y(dy), 2) * NX + at_x(dx)
            arrived(slots.at[place], recv.at[place])
            arrived(slots.at[0], send.at[k])

    def exchange2(slots, send, recv):
        for dz in range(1, NZ):
            remote(slots.at[z], slots.at[z], send.at[dz - 1], recv.at[z], {"z": at_z(dz)})

    def wait2(slots, send, recv):
        for dz in range(1, NZ):
            arrived(slots.at[at_z(dz)], recv.at[at_z(dz)])
            arrived(slots.at[0], send.at[dz - 1])

    def summed(slots):
        total = slots[0]
        for k in range(1, 8):
            total = total + slots[k]
        return total

    stat1[me1] = norm[...]
    exchange1(stat1, s1_send, s1_recv)
    hit1[me1] = hit[...]
    exchange1(hit1, h1_send, h1_recv)
    wait1(stat1, s1_send, s1_recv)
    stat2[z] = log_sum_exp([stat1[k] for k in range(8)])
    exchange2(stat2, s2_send, s2_recv)
    wait2(stat2, s2_send, s2_recv)
    norm[...] = log_sum_exp([stat2[k] for k in range(8)])

    wait1(hit1, h1_send, h1_recv)
    here = lax.rem(lax.div(chosen[...], OWN * NY * NC), NZ) == z
    missed = jnp.where(here, norm[...] - summed(hit1), 0.0)
    loss2[z] = missed[:8] + missed[8:]
    exchange2(loss2, h2_send, h2_recv)

    def make_weights(some):
        def tile_weights(j, carry):
            start = pl.multiple_of(j * 128, 128)
            log_norm = norm[pl.ds(j, 1), :]
            ids = chosen[pl.ds(j, 1), :]
            for place, lists, first in some:
                soft = jnp.exp(logits[pl.ds(place, lists), pl.ds(start, 128)] - log_norm)
                soft = jnp.where(sub[:lists] == ids - first, soft - 1.0, soft)
                weights[pl.ds(place, lists), pl.ds(start, 128)] = soft.astype(jnp.bfloat16)
            return carry

        lax.fori_loop(0, TILES, tile_weights, 0)

    def pair_gradient(first, n):
        part[n, first * OWN : (first + 2) * OWN, :] = jnp.dot(
            weights[first * OWN : (first + 2) * OWN, :],
            q[:, :, :, n * WIDTH : (n + 1) * WIDTH].reshape(DEV_ROWS, WIDTH),
            preferred_element_type=jnp.float32,
        )

    to_partner, to_owner = [], []

    def hand_over(n, slot):
        lists = part.at[n, pl.ds((1 + 2 * slot) * OWN, OWN)]
        to_partner.append(remote(lists, from_partner.at[n, slot], d_send.at[n, slot], d_recv.at[n, slot], partner))

    def give_back(n):
        arrived(from_partner.at[n, 1], d_recv.at[n, 1])
        y_out[n] = part[n, 2 * OWN : 3 * OWN, :] + from_partner[n, 1]
        for h, k in enumerate((-1, 1)):
            source, target = y_out.at[n, pl.ds(h * HALF, HALF)], y_in.at[n, pl.ds(h * HALF, HALF)]
            to_owner.append(remote(source, target, y_send.at[n, h], y_recv.at[n, h], {"y": at_y(k)}))

    make_weights(parts[2:])
    for n in range(PARTS):
        pair_gradient(2, n)
        hand_over(n, 1)
    make_weights(parts[:2])
    for n in range(PARTS):
        give_back(n)
    wait2(loss2, h2_send, h2_recv)
    loss[0] = summed(loss2)
    loss_across = remote(loss.at[0], loss.at[1], l_send.at[0], l_recv.at[0], partner)
    for n in range(PARTS):
        pair_gradient(0, n)
        hand_over(n, 0)
    loss_across.wait()
    loss[2] = loss[0] + loss[1]
    loss_back = remote(loss.at[2], loss.at[3], l_send.at[1], l_recv.at[1], {"y": at_y(1)})
    for n in range(PARTS):
        arrived(from_partner.at[n, 0], d_recv.at[n, 0])
        for h in range(2):
            arrived(y_in.at[n, pl.ds(h * HALF, HALF)], y_recv.at[n, h])
        grad_ref[:, n * WIDTH : (n + 1) * WIDTH] = part[n, :OWN, :] + from_partner[n, 0] + y_in[n]
    loss_back.wait()
    loss_ref[...] = jnp.sum(loss[2] + loss[3], keepdims=True) * (1.0 / ROWS)

    for k in range(SENDS):
        arrived(q.at[0, 0], q_send.at[k])
    for copy in table_sends + to_partner + to_owner:
        copy.wait_send()


def shards(query_emb, positive_list, centroids, first_moment, second_moment):
    f32, bf16, i32, dma = jnp.float32, jnp.bfloat16, jnp.int32, pltpu.SemaphoreType.DMA
    vmem, hbm = pl.BlockSpec(memory_space=pltpu.VMEM), pl.BlockSpec(memory_space=pl.ANY)
    gradient, loss = pl.pallas_call(
        kernel,
        name="step",
        out_shape=(jax.ShapeDtypeStruct((OWN, D), f32), jax.ShapeDtypeStruct((1, 1), f32)),
        in_specs=[hbm, hbm, hbm],
        out_specs=(vmem, vmem),
        scratch_shapes=[
            pltpu.VMEM((BLOCKS, PIECES, PIECE, D), bf16),
            pltpu.VMEM((ROWS // 128, 128), i32),
            pltpu.VMEM((OWN, D), f32),
            pltpu.VMEM((TILES, 128), i32),
            pltpu.VMEM((HELD, D), bf16),
            pltpu.VMEM((HELD, DEV_ROWS), f32),
            pltpu.VMEM((HELD, DEV_ROWS), bf16),
            pltpu.VMEM((TILES, 128), f32),
            pltpu.VMEM((TILES, 128), f32),
            pltpu.VMEM((8, TILES, 128), f32),
            pltpu.VMEM((8, TILES, 128), f32),
            pltpu.VMEM((8, TILES, 128), f32),
            pltpu.VMEM((8, 8, 128), f32),
            pltpu.VMEM((4, 8, 128), f32),
            pltpu.VMEM((PARTS, HELD, WIDTH), f32),
            pltpu.VMEM((PARTS, 2, OWN, WIDTH), f32),
            pltpu.VMEM((PARTS, OWN, WIDTH), f32),
            pltpu.VMEM((PARTS, OWN, WIDTH), f32),
            dma((PIECES + 2,)), dma((SENDS,)), dma((BLOCKS * PIECES,)), dma((5,)), dma((5,)),
            dma((7,)), dma((8,)), dma((7,)), dma((8,)), dma((7,)), dma((8,)), dma((7,)), dma((8,)), dma((2,)), dma((2,)),
            dma((PARTS, 2)), dma((PARTS, 2)), dma((PARTS, 2)), dma((PARTS, 2)),
        ],
        compiler_params=pltpu.CompilerParams(collective_id=0, has_side_effects=True, vmem_limit_bytes=56000000),
    )(query_emb, positive_list.reshape(ROWS // 128, 128), centroids)
    return (*adam_update(centroids, first_moment, second_moment, gradient), loss[0, 0])


def solution(mesh):
    split = Mesh(mesh.devices.reshape(NX, NZ, NY, NC), AXES)
    placed = (P(DP, None), P(), P(DP_MP, None), P(DP_MP, None), P(DP_MP, None))
    return jax.shard_map(
        shards,
        mesh=split,
        in_specs=placed,
        out_specs=(P(DP_MP, None), P(DP_MP, None), P(DP_MP, None), P()),
        check_vma=False,
    )
```

```python
import jax
import jax.numpy as jnp
from jax import lax
from jax.experimental import pallas as pl
from jax.experimental.pallas import tpu as pltpu
from jax.sharding import Mesh
from jax.sharding import PartitionSpec as P

NX, NZ, NY, NC = 4, 8, 4, 2
AXES = ("x", "z", "y", "c")
DP = ("x", "z")
DP_MP = ("x", "z", "y", "c")
MESH = pl.DeviceIdType.MESH

ROWS = 8192
D = 768
LISTS = 32768
BLOCKS = NX * NZ
CLASSES = 4
BLOCK_ROWS = ROWS // BLOCKS // CLASSES
DEV_ROWS = BLOCKS * BLOCK_ROWS
OWN = LISTS // (NX * NZ * NY * NC)
HELD = 4 * OWN
TILES = DEV_ROWS // 128
GROUP = 4 * BLOCK_ROWS
PIECES = 2
PIECE = BLOCK_ROWS // PIECES
SENDS = 31 * PIECES
HALF = OWN // 2
PARTS = 3
WIDTH = D // PARTS

beta_first = 0.9
beta_second = 0.95
learn_rate = 0.01
epsilon = 1e-08


def adam_update(centroids, first_moment, second_moment, gradient):
    new_first = beta_first * first_moment + (1.0 - beta_first) * gradient
    new_second = beta_second * second_moment + (1.0 - beta_second) * gradient * gradient
    new_centroids = centroids - learn_rate * new_first / (jnp.sqrt(new_second) + epsilon)
    return (new_centroids, new_first, new_second)


def log_sum_exp(slots):
    top = slots[0]
    for part in slots[1:]:
        top = jnp.maximum(top, part)
    total = jnp.exp(slots[0] - top)
    for part in slots[1:]:
        total = total + jnp.exp(part - top)
    return top + jnp.log(total)


STARTS = [('UDrRL', 'uDdLUR'), ('UDRL', 'UDLR')]
CUTS = ((17, 31, 35, 46, 49, 51, 55, 62), (19, 29, 33, 47, 49, 52, 55, 62))
GROUPS = ((0, -1, 1, 3, -2, 2, -3, 4), (0, -1, 1, -2, 2, -3, 3, 4))
ROUTES = (
    (
        (0, -1, 0, "UL"), (0, 1, 0, "DRL"), (1, 0, 1, "LU"), (0, 1, 1, "RL"), (2, 0, 0, "D"), (-1, 0, 0, "U"),
        (0, -2, 1, "RUL"), (0, -1, 1, "R"), (0, 2, 1, "DL"), (0, -2, 0, "RU"), (1, -1, 0, "UL"), (0, 2, 0, "DRL"),
        (-1, 1, 1, "DR"), (2, 1, 0, "d"), (2, 0, 1, "U"), (1, 0, 0, ""), (-1, 0, 1, ""), (-1, -2, 1, "U"),
        (0, 3, 1, "rRD"), (0, -3, 1, "L"), (0, 3, 0, "DL"), (-1, -2, 0, "UR"), (1, 2, 1, "D"), (-1, 2, 1, "R"),
        (1, -2, 0, "U"), (-1, 2, 0, "D"), (2, -1, 1, "U"), (1, -1, 1, ""), (-1, -1, 0, ""), (-1, -1, 1, ""),
        (2, -1, 0, ""), (-1, 1, 0, ""), (1, 1, 0, ""), (1, 1, 1, ""), (2, 1, 1, ""), (1, 2, 0, "L"), (2, 3, 0, "D"),
        (-1, -3, 1, "U"), (1, -3, 1, "UL"), (-1, -3, 0, "R"), (0, 4, 0, "RL"), (2, 3, 1, "D"), (-1, 3, 1, ""),
        (1, 3, 0, ""), (1, 3, 1, ""), (-1, 3, 0, ""), (1, -2, 1, ""), (2, -2, 0, ""), (2, -2, 1, ""), (2, 2, 1, ""),
        (2, 2, 0, ""), (0, -3, 0, ""), (1, -3, 0, ""), (2, -3, 1, ""), (2, -3, 0, ""), (0, 4, 1, ""), (2, 4, 0, ""),
        (-1, 4, 1, ""), (1, 4, 0, ""), (2, 4, 1, ""), (-1, 4, 0, ""), (1, 4, 1, ""),
    ),
    (
        (-1, 0, 0, "DR"), (1, 0, 0, "d"), (0, -1, 0, "LUR"), (0, 1, 0, "DL"), (-1, 0, 1, "DR"), (1, 0, 1, "D"),
        (0, -1, 1, "uRLU"), (0, 1, 1, "D"), (1, -1, 0, "uL"), (0, -2, 0, "RUL"), (-1, 1, 0, "R"), (1, -1, 1, "U"),
        (1, 2, 0, "L"), (0, 2, 0, "RD"), (0, -3, 1, "L"), (-1, -1, 1, "UR"), (-1, -2, 0, "UR"), (2, 0, 0, ""),
        (2, 0, 1, ""), (1, 1, 1, "L"), (0, 2, 1, "DRL"), (1, -3, 0, "LU"), (-1, 2, 0, "D"), (1, -3, 1, "UL"),
        (0, -3, 0, "U"), (0, 3, 0, "L"), (-1, -1, 0, ""), (2, -1, 0, ""), (2, -1, 1, ""), (1, 1, 0, ""),
        (-1, 1, 1, ""), (2, 1, 0, ""), (2, 1, 1, ""), (1, -2, 1, "L"), (1, 2, 1, "D"), (0, 3, 1, "RD"),
        (-1, -2, 1, "U"), (-1, 2, 1, "R"), (2, -3, 0, "U"), (-1, 3, 0, "D"), (1, 3, 0, "L"), (-1, 3, 1, "DR"),
        (1, 4, 1, "L"), (0, -2, 1, ""), (1, -2, 0, ""), (2, -2, 0, ""), (2, -2, 1, ""), (2, 2, 0, ""), (2, 2, 1, ""),
        (-1, -3, 0, ""), (2, -3, 1, ""), (-1, -3, 1, ""), (1, 3, 1, ""), (2, 3, 0, ""), (2, 3, 1, ""), (1, 4, 0, ""),
        (0, 4, 1, ""), (0, 4, 0, ""), (-1, 4, 0, ""), (-1, 4, 1, ""), (2, 4, 0, ""), (2, 4, 1, ""),
    ),
)


def kernel(
    query_hbm, pos_hbm, cent_hbm, grad_hbm, loss_ref,
    q, pos, cent, chosen, table, logits, weights, norm, hit, stat1, stat2, hit1, loss2, loss,
    part, from_partner, y_out, y_in, grad,
    own_sem, q_send, q_recv, t_send, t_recv,
    s1_send, s1_recv, s2_send, s2_recv, h1_send, h1_recv, h2_send, h2_recv, l_send, l_recv,
    d_send, d_recv, y_send, y_recv, g_sem,
):
    x, z, y, c = (lax.axis_index(a) for a in AXES)

    def at_x(k):
        return lax.rem(x + (k + NX), NX)

    def at_z(k):
        return lax.rem(z + (k + NZ), NZ)

    def at_y(k):
        return lax.rem(y + (k + NY), NY)

    other = 1 - c
    partner = {"c": other}

    group1 = [(2, 2), (1, 2), (3, 2), (0, 2), (2, 0), (1, 0), (3, 0)]
    peers = [{"x": at_x(k)} for k in (1, -1, 2)] + [{"z": at_z(k)} for k in (1, -1, 2, -2)]
    peers += [partner] + [{"y": at_y(k), "c": core} for k in (1, -1) for core in (c, other)]
    group2 = (4, 3, 5, 2, 6, 1, 7)
    barrier = pltpu.get_barrier_semaphore()
    for peer in peers:
        pl.semaphore_signal(barrier, inc=1, device_id=peer, device_id_type=MESH)

    def remote(src, dst, send, recv, where):
        copy = pltpu.make_async_remote_copy(
            src_ref=src, dst_ref=dst, send_sem=send, recv_sem=recv, device_id=where, device_id_type=MESH
        )
        copy.start()
        return copy

    def arrived(dst, sem):
        pltpu.make_async_copy(dst, dst, sem).wait()

    row_class = lax.rem(y, 2) * 2 + c
    own_place = z * NX + x
    local = [
        pltpu.make_async_copy(
            query_hbm.at[pl.ds(pl.multiple_of(row_class * BLOCK_ROWS + p * PIECE, PIECE), PIECE)],
            q.at[own_place, p],
            own_sem.at[p],
        )
        for p in range(PIECES)
    ]
    local.append(pltpu.make_async_copy(cent_hbm, cent, own_sem.at[PIECES]))
    local.append(pltpu.make_async_copy(pos_hbm, pos, own_sem.at[PIECES + 1]))
    for copy in local:
        copy.start()
    pl.semaphore_wait(barrier, len(peers))
    for copy in local[:PIECES]:
        copy.wait()

    toward = {"R": {"x": at_x(1)}, "L": {"x": at_x(-1)}, "U": {"z": at_z(1)}, "D": {"z": at_z(-1)}}
    toward |= {"r": {"x": at_x(2)}, "l": {"x": at_x(2)}, "u": {"z": at_z(2)}, "d": {"z": at_z(-2)}}

    def carrier():
        count = [0]

        def send(dx, dz, p, links):
            place = at_z(dz) * NX + at_x(dx)
            for link in links:
                remote(q.at[place, p], q.at[place, p], q_send.at[count[0]], q_recv.at[place * PIECES + p], toward[link])
                count[0] += 1

        return send, count

    carriers = [carrier() for _ in range(NC)]

    def move(r):
        for core in range(NC):
            send, _ = carriers[core]
            cuts = (0, *CUTS[core])
            events = ROUTES[core][cuts[r] : cuts[r + 1]]

            @pl.when(c == core)
            def _(send=send, core=core, events=events):
                for dx, dz, p, links in events:
                    place = at_z(dz) * NX + at_x(dx)
                    arrived(q.at[place, p], q_recv.at[place * PIECES + p])
                    send(dx, dz, p, links)

    parity = lax.rem(y, 2)
    lane = lax.broadcasted_iota(jnp.int32, (1, 128), 1)

    def targets(bz, bx):
        return pos[pl.ds((bx * NZ + bz) * 2 + parity, 1), :]

    def choose():
        for j in range(TILES):
            r0, r1 = targets(j // 2, 2 * (j % 2)), targets(j // 2, 2 * (j % 2) + 1)
            low = jnp.where(c == 0, r0, pltpu.roll(r0, 64, 1))
            high = jnp.where(c == 0, pltpu.roll(r1, 64, 1), r1)
            chosen[j : j + 1, :] = jnp.where(lane < 64, low, high)

    sub = lax.broadcasted_iota(jnp.int32, (OWN, 128), 0)
    first_block = (x * NZ + z) * NY * NC
    held = [(0, OWN, y, c, 0), (OWN, OWN, y, other, 0)]
    for place, core in ((2 * OWN, c), (3 * OWN, other)):
        held += [(place, HALF, at_y(-1), core, 0), (place + HALF, HALF, at_y(1), core, HALF)]
    parts = [(place, lists, (first_block + hy * NC + hc) * OWN + first) for place, lists, hy, hc, first in held]

    def group_logits(r):
        group = jnp.where(c == 0, at_z(GROUPS[0][r]), at_z(GROUPS[1][r]))
        start = pl.multiple_of(group * GROUP, GROUP)
        rows = q[pl.ds(group * NX, NX)].reshape(GROUP, D)
        block = lax.dot_general(
            table[...], rows, (((1,), (1,)), ((), ())), preferred_element_type=jnp.float32
        )
        logits[:, pl.ds(start, GROUP)] = block
        peak = jnp.max(block, axis=0, keepdims=True)
        mass = jnp.sum(jnp.exp(block - peak), axis=0, keepdims=True)
        local_norm = peak + jnp.log(mass)
        for h in range(2):
            tile = group * 2 + h
            norm[pl.ds(tile, 1), :] = local_norm[:, h * 128 : h * 128 + 128]
            ids = chosen[pl.ds(tile, 1), :]
            found = jnp.zeros((1, 128), jnp.float32)
            for place, lists, first in parts:
                values = block[place : place + lists, h * 128 : h * 128 + 128]
                found = found + jnp.sum(jnp.where(sub[:lists] == ids - first, values, 0.0), axis=0, keepdims=True)
            hit[pl.ds(tile, 1), :] = found

    table_sends = []
    table_routes = [
        (0, 2 * OWN, HALF, {"y": at_y(1)}),
        (1, 2 * OWN + HALF, HALF, {"y": at_y(-1)}),
        (0, 3 * OWN, HALF, {"y": at_y(1), "c": other}),
        (1, 3 * OWN + HALF, HALF, {"y": at_y(-1), "c": other}),
        (0, OWN, OWN, partner),
    ]

    def share_table():
        local[PIECES].wait()
        table[:OWN, :] = cent[...].astype(jnp.bfloat16)
        for k, (half, place, rows, where) in enumerate(table_routes):
            source, target = table.at[pl.ds(half * HALF, rows)], table.at[pl.ds(place, rows)]
            table_sends.append(remote(source, target, t_send.at[k], t_recv.at[k], where))

    for core in range(NC):
        send, _ = carriers[core]

        @pl.when(c == core)
        def _(send=send, core=core):
            for p in range(PIECES):
                send(0, 0, p, STARTS[core][p])

    share_table()
    local[PIECES + 1].wait()
    for r in range(8):
        move(r)
        if r == 0:
            choose()
            for k, (_, place, rows, _) in enumerate(table_routes):
                arrived(table.at[pl.ds(place, rows)], t_recv.at[k])
        group_logits(r)
    for _, count in carriers:
        assert count[0] == SENDS

    me1 = lax.div(y, 2) * NX + x

    def exchange1(slots, send, recv):
        for k, (dx, dy) in enumerate(group1):
            remote(slots.at[me1], slots.at[me1], send.at[k], recv.at[me1], {"x": at_x(dx), "y": at_y(dy)})

    def wait1(slots, send, recv):
        for dx, dy in group1:
            place = lax.div(at_y(dy), 2) * NX + at_x(dx)
            arrived(slots.at[place], recv.at[place])

    def exchange2(slots, send, recv):
        for k, dz in enumerate(group2):
            remote(slots.at[z], slots.at[z], send.at[k], recv.at[z], {"z": at_z(dz)})

    def wait2(slots, send, recv):
        for dz in group2:
            arrived(slots.at[at_z(dz)], recv.at[at_z(dz)])

    def summed(slots):
        total = slots[0]
        for k in range(1, 8):
            total = total + slots[k]
        return total

    stat1[me1] = norm[...]
    exchange1(stat1, s1_send, s1_recv)
    hit1[me1] = hit[...]
    exchange1(hit1, h1_send, h1_recv)
    wait1(stat1, s1_send, s1_recv)
    stat2[z] = log_sum_exp([stat1[k] for k in range(8)])
    exchange2(stat2, s2_send, s2_recv)
    wait2(stat2, s2_send, s2_recv)
    norm[...] = log_sum_exp([stat2[k] for k in range(8)])

    wait1(hit1, h1_send, h1_recv)
    here = lax.rem(lax.div(chosen[...], OWN * NY * NC), NZ) == z
    missed = jnp.where(here, norm[...] - summed(hit1), 0.0)
    loss2[z] = missed[:8] + missed[8:]
    exchange2(loss2, h2_send, h2_recv)

    def make_weights(some):
        def tile_weights(j, carry):
            start = pl.multiple_of(j * 128, 128)
            log_norm = norm[pl.ds(j, 1), :]
            ids = chosen[pl.ds(j, 1), :]
            for place, lists, first in some:
                soft = jnp.exp(logits[pl.ds(place, lists), pl.ds(start, 128)] - log_norm)
                soft = jnp.where(sub[:lists] == ids - first, soft - 1.0, soft)
                weights[pl.ds(place, lists), pl.ds(start, 128)] = soft.astype(jnp.bfloat16)
            return carry

        lax.fori_loop(0, TILES, tile_weights, 0)

    def pair_gradient(first, n):
        part[n, first * OWN : (first + 2) * OWN, :] = jnp.dot(
            weights[first * OWN : (first + 2) * OWN, :],
            q[:, :, :, n * WIDTH : (n + 1) * WIDTH].reshape(DEV_ROWS, WIDTH),
            preferred_element_type=jnp.float32,
        )

    to_partner, to_owner, outs = [], [], []

    def hand_over(n, slot):
        lists = part.at[n, pl.ds((1 + 2 * slot) * OWN, OWN)]
        to_partner.append(remote(lists, from_partner.at[n, slot], d_send.at[n, slot], d_recv.at[n, slot], partner))

    def give_back(n):
        arrived(from_partner.at[n, 1], d_recv.at[n, 1])
        y_out[n] = part[n, 2 * OWN : 3 * OWN, :] + from_partner[n, 1]
        for h, k in enumerate((-1, 1)):
            source, target = y_out.at[n, pl.ds(h * HALF, HALF)], y_in.at[n, pl.ds(h * HALF, HALF)]
            to_owner.append(remote(source, target, y_send.at[n, h], y_recv.at[n, h], {"y": at_y(k)}))

    make_weights(parts[2:])
    for n in range(PARTS):
        pair_gradient(2, n)
        hand_over(n, 1)
    make_weights(parts[:2])
    for n in range(PARTS):
        give_back(n)
    wait2(loss2, h2_send, h2_recv)
    loss[0] = summed(loss2)
    loss_across = remote(loss.at[0], loss.at[1], l_send.at[0], l_recv.at[0], partner)
    for n in range(PARTS):
        pair_gradient(0, n)
        hand_over(n, 0)
    loss_across.wait()
    loss[2] = loss[0] + loss[1]
    loss_back = remote(loss.at[2], loss.at[3], l_send.at[1], l_recv.at[1], {"y": at_y(1)})
    for n in range(PARTS):
        arrived(from_partner.at[n, 0], d_recv.at[n, 0])
        for h in range(2):
            arrived(y_in.at[n, pl.ds(h * HALF, HALF)], y_recv.at[n, h])
        grad[n] = part[n, :OWN, :] + from_partner[n, 0] + y_in[n]
        out = pltpu.make_async_copy(grad.at[n], grad_hbm.at[:, pl.ds(n * WIDTH, WIDTH)], g_sem.at[n])
        out.start()
        outs.append(out)
    loss_back.wait()
    loss_ref[...] = jnp.sum(loss[2] + loss[3], keepdims=True) * (1.0 / ROWS)

    for k in range(SENDS):
        arrived(q.at[0, 0], q_send.at[k])
    for slots, send in ((stat1, s1_send), (hit1, h1_send), (stat2, s2_send), (loss2, h2_send)):
        for k in range(7):
            arrived(slots.at[0], send.at[k])
    for copy in table_sends + to_partner + to_owner:
        copy.wait_send()
    for copy in outs:
        copy.wait()


def shards(query_emb, positive_list, centroids, first_moment, second_moment):
    f32, bf16, i32, dma = jnp.float32, jnp.bfloat16, jnp.int32, pltpu.SemaphoreType.DMA
    vmem, hbm = pl.BlockSpec(memory_space=pltpu.VMEM), pl.BlockSpec(memory_space=pl.ANY)
    gradient, loss = pl.pallas_call(
        kernel,
        name="step",
        out_shape=(jax.ShapeDtypeStruct((OWN, D), f32), jax.ShapeDtypeStruct((1, 1), f32)),
        in_specs=[hbm, hbm, hbm],
        out_specs=(hbm, vmem),
        scratch_shapes=[
            pltpu.VMEM((BLOCKS, PIECES, PIECE, D), bf16),
            pltpu.VMEM((ROWS // 128, 128), i32),
            pltpu.VMEM((OWN, D), f32),
            pltpu.VMEM((TILES, 128), i32),
            pltpu.VMEM((HELD, D), bf16),
            pltpu.VMEM((HELD, DEV_ROWS), f32),
            pltpu.VMEM((HELD, DEV_ROWS), bf16),
            pltpu.VMEM((TILES, 128), f32),
            pltpu.VMEM((TILES, 128), f32),
            pltpu.VMEM((8, TILES, 128), f32),
            pltpu.VMEM((8, TILES, 128), f32),
            pltpu.VMEM((8, TILES, 128), f32),
            pltpu.VMEM((8, 8, 128), f32),
            pltpu.VMEM((4, 8, 128), f32),
            pltpu.VMEM((PARTS, HELD, WIDTH), f32),
            pltpu.VMEM((PARTS, 2, OWN, WIDTH), f32),
            pltpu.VMEM((PARTS, OWN, WIDTH), f32),
            pltpu.VMEM((PARTS, OWN, WIDTH), f32),
            pltpu.VMEM((PARTS, OWN, WIDTH), f32),
            dma((PIECES + 2,)), dma((SENDS,)), dma((BLOCKS * PIECES,)), dma((5,)), dma((5,)),
            dma((7,)), dma((8,)), dma((7,)), dma((8,)), dma((7,)), dma((8,)), dma((7,)), dma((8,)), dma((2,)), dma((2,)),
            dma((PARTS, 2)), dma((PARTS, 2)), dma((PARTS, 2)), dma((PARTS, 2)), dma((PARTS,)),
        ],
        compiler_params=pltpu.CompilerParams(collective_id=0, has_side_effects=True, vmem_limit_bytes=65800000),
    )(query_emb, positive_list.reshape(ROWS // 128, 128), centroids)
    return (*adam_update(centroids, first_moment, second_moment, gradient), loss[0, 0])


def solution(mesh):
    split = Mesh(mesh.devices.reshape(NX, NZ, NY, NC), AXES)
    placed = (P(DP, None), P(), P(DP_MP, None), P(DP_MP, None), P(DP_MP, None))
    return jax.shard_map(
        shards,
        mesh=split,
        in_specs=placed,
        out_specs=(P(DP_MP, None), P(DP_MP, None), P(DP_MP, None), P()),
        check_vma=False,
    )
```

```python
import jax
import jax.numpy as jnp
from jax import lax
from jax.experimental import pallas as pl
from jax.experimental.pallas import tpu as pltpu
from jax.sharding import Mesh
from jax.sharding import PartitionSpec as P

NX, NZ, NY, NC = 4, 8, 4, 2
AXES = ("x", "z", "y", "c")
DP = ("x", "z")
DP_MP = ("x", "z", "y", "c")
MESH = pl.DeviceIdType.MESH

ROWS = 8192
D = 768
LISTS = 32768
BLOCKS = NX * NZ
CLASSES = 4
BLOCK_ROWS = ROWS // BLOCKS // CLASSES
DEV_ROWS = BLOCKS * BLOCK_ROWS
OWN = LISTS // (NX * NZ * NY * NC)
HELD = 4 * OWN
TILES = DEV_ROWS // 128
GROUP = 4 * BLOCK_ROWS
PIECES = 2
PIECE = BLOCK_ROWS // PIECES
SENDS = 31 * PIECES
HALF = OWN // 2
PARTS = 3
WIDTH = D // PARTS

beta_first = 0.9
beta_second = 0.95
learn_rate = 0.01
epsilon = 1e-08


def adam_update(centroids, first_moment, second_moment, gradient):
    new_first = beta_first * first_moment + (1.0 - beta_first) * gradient
    new_second = beta_second * second_moment + (1.0 - beta_second) * gradient * gradient
    new_centroids = centroids - learn_rate * new_first / (jnp.sqrt(new_second) + epsilon)
    return (new_centroids, new_first, new_second)


def log_sum_exp(slots):
    top = slots[0]
    for part in slots[1:]:
        top = jnp.maximum(top, part)
    total = jnp.exp(slots[0] - top)
    for part in slots[1:]:
        total = total + jnp.exp(part - top)
    return top + jnp.log(total)


STARTS = [('UDLR', 'RuUdDrL'), ('UDRL', 'UDLR')]
CUTS = ((17, 30, 41, 45, 48, 53, 57, 62), (18, 26, 32, 42, 49, 52, 56, 62))
GROUPS = ((0, 1, 2, -1, -2, 3, -3, 4), (0, -1, 1, -2, 2, -3, 3, 4))
ROUTES = (
    (
        (1, 0, 0, "DL"), (0, -1, 0, "uURL"), (0, 1, 0, "DrR"), (-1, 0, 1, "D"), (0, -2, 1, "ULr"), (0, 2, 1, "DL"),
        (0, -1, 1, "RL"), (0, 1, 1, "L"), (2, 0, 1, "D"), (2, 0, 0, "U"), (1, 1, 0, "D"), (0, 2, 0, "D"),
        (0, -3, 0, "RUL"), (0, -2, 0, "RL"), (-1, 1, 1, "D"), (-1, 0, 0, ""), (1, 0, 1, ""), (2, 1, 0, "D"),
        (1, -2, 1, "U"), (-1, 1, 0, "D"), (0, -3, 1, "U"), (0, 3, 1, "r"), (1, 2, 1, "DL"), (-1, -1, 1, "U"),
        (1, -1, 1, "L"), (1, 2, 0, "D"), (-1, -3, 0, "UR"), (0, 4, 0, "L"), (2, 1, 1, ""), (1, 1, 1, ""),
        (0, 3, 0, "R"), (-1, -2, 0, "R"), (1, -3, 1, "UL"), (-1, 2, 1, "D"), (0, 4, 1, "R"), (2, 2, 0, "D"),
        (-1, -2, 1, "U"), (2, 3, 1, "D"), (-1, 4, 0, "R"), (2, 2, 1, ""), (-1, 2, 0, ""), (-1, -1, 0, ""),
        (1, -1, 0, ""), (2, -1, 0, ""), (2, -1, 1, ""), (2, -2, 1, ""), (1, -2, 0, ""), (2, -2, 0, ""),
        (1, 3, 1, ""), (-1, 3, 0, ""), (1, 3, 0, ""), (-1, 3, 1, ""), (2, 3, 0, ""), (1, -3, 0, ""), (2, -3, 0, ""),
        (2, -3, 1, ""), (-1, -3, 1, ""), (1, 4, 1, ""), (1, 4, 0, ""), (-1, 4, 1, ""), (2, 4, 1, ""), (2, 4, 0, ""),
    ),
    (
        (-1, 0, 0, "DR"), (0, -1, 0, "RUL"), (0, 1, 0, "DL"), (-1, 0, 1, "D"), (1, 0, 1, "UL"), (0, -1, 1, "UR"),
        (0, 1, 1, "DL"), (2, 0, 0, "U"), (0, -2, 0, "UL"), (-1, 1, 0, "D"), (-1, -1, 0, "U"), (1, 1, 0, "DL"),
        (0, 2, 0, "D"), (1, -1, 1, "uL"), (2, 0, 1, "D"), (0, -2, 1, "URL"), (0, 2, 1, "RDL"), (1, 0, 0, ""),
        (-1, 2, 0, "R"), (0, -3, 0, "L"), (-1, -2, 0, "UR"), (-1, -2, 1, "R"), (1, -1, 0, ""), (-1, -1, 1, ""),
        (2, -1, 0, ""), (2, -1, 1, ""), (0, 3, 0, "DLR"), (-1, 2, 1, "D"), (2, 1, 1, "D"), (-1, 1, 1, ""),
        (1, 1, 1, ""), (2, 1, 0, ""), (1, -3, 1, "LU"), (0, 3, 1, "L"), (0, -3, 1, "UR"), (2, -2, 0, "u"),
        (1, -3, 0, "L"), (0, 4, 0, "L"), (-1, -3, 0, "U"), (1, -2, 0, ""), (1, -2, 1, ""), (2, -2, 1, ""),
        (1, 3, 0, "L"), (-1, 3, 1, "R"), (2, -3, 1, "U"), (1, 2, 0, ""), (2, 2, 0, ""), (1, 2, 1, ""), (2, 2, 1, ""),
        (0, 4, 1, "R"), (-1, -3, 1, ""), (2, -3, 0, ""), (-1, 3, 0, ""), (1, 3, 1, ""), (2, 3, 1, ""), (2, 3, 0, ""),
        (1, 4, 1, ""), (1, 4, 0, ""), (2, 4, 0, ""), (-1, 4, 0, ""), (2, 4, 1, ""), (-1, 4, 1, ""),
    ),
)


def kernel(
    query_hbm, pos_hbm, cent_hbm, grad_hbm, loss_ref,
    q, pos, cent, chosen, table, logits, weights, norm, hit, stat1, stat2, hit1, loss2, loss,
    part, from_partner, y_out, y_in, grad,
    own_sem, q_send, q_recv, t_send, t_recv,
    s1_send, s1_recv, s2_send, s2_recv, h1_send, h1_recv, h2_send, h2_recv, l_send, l_recv,
    d_send, d_recv, y_send, y_recv, g_sem,
):
    x, z, y, c = (lax.axis_index(a) for a in AXES)

    def at_x(k):
        return lax.rem(x + (k + NX), NX)

    def at_z(k):
        return lax.rem(z + (k + NZ), NZ)

    def at_y(k):
        return lax.rem(y + (k + NY), NY)

    other = 1 - c
    partner = {"c": other}

    group1 = [(2, 2), (1, 2), (3, 2), (0, 2), (2, 0), (1, 0), (3, 0)]
    peers = [{"x": at_x(k)} for k in (1, -1, 2)] + [{"z": at_z(k)} for k in (1, -1, 2, -2)]
    peers += [partner] + [{"y": at_y(k), "c": core} for k in (1, -1) for core in (c, other)]
    group2 = (4, 3, 5, 2, 6, 1, 7)
    barrier = pltpu.get_barrier_semaphore()
    for peer in peers:
        pl.semaphore_signal(barrier, inc=1, device_id=peer, device_id_type=MESH)

    def remote(src, dst, send, recv, where):
        copy = pltpu.make_async_remote_copy(
            src_ref=src, dst_ref=dst, send_sem=send, recv_sem=recv, device_id=where, device_id_type=MESH
        )
        copy.start()
        return copy

    def arrived(dst, sem):
        pltpu.make_async_copy(dst, dst, sem).wait()

    row_class = lax.rem(y, 2) * 2 + c
    own_place = z * NX + x
    local = [
        pltpu.make_async_copy(
            query_hbm.at[pl.ds(pl.multiple_of(row_class * BLOCK_ROWS + p * PIECE, PIECE), PIECE)],
            q.at[own_place, p],
            own_sem.at[p],
        )
        for p in range(PIECES)
    ]
    local.append(pltpu.make_async_copy(cent_hbm, cent, own_sem.at[PIECES]))
    local.append(pltpu.make_async_copy(pos_hbm, pos, own_sem.at[PIECES + 1]))
    for copy in local:
        copy.start()
    pl.semaphore_wait(barrier, len(peers))
    for copy in local[:PIECES]:
        copy.wait()

    toward = {"R": {"x": at_x(1)}, "L": {"x": at_x(-1)}, "U": {"z": at_z(1)}, "D": {"z": at_z(-1)}}
    toward |= {"r": {"x": at_x(2)}, "l": {"x": at_x(2)}, "u": {"z": at_z(2)}, "d": {"z": at_z(-2)}}

    def carrier():
        count = [0]

        def send(dx, dz, p, links):
            place = at_z(dz) * NX + at_x(dx)
            for link in links:
                remote(q.at[place, p], q.at[place, p], q_send.at[count[0]], q_recv.at[place * PIECES + p], toward[link])
                count[0] += 1

        return send, count

    carriers = [carrier() for _ in range(NC)]

    def move(r):
        for core in range(NC):
            send, _ = carriers[core]
            cuts = (0, *CUTS[core])
            events = ROUTES[core][cuts[r] : cuts[r + 1]]

            @pl.when(c == core)
            def _(send=send, core=core, events=events):
                for dx, dz, p, links in events:
                    place = at_z(dz) * NX + at_x(dx)
                    arrived(q.at[place, p], q_recv.at[place * PIECES + p])
                    send(dx, dz, p, links)

    parity = lax.rem(y, 2)
    lane = lax.broadcasted_iota(jnp.int32, (1, 128), 1)

    def targets(bz, bx):
        return pos[pl.ds((bx * NZ + bz) * 2 + parity, 1), :]

    def choose():
        for j in range(TILES):
            r0, r1 = targets(j // 2, 2 * (j % 2)), targets(j // 2, 2 * (j % 2) + 1)
            low = jnp.where(c == 0, r0, pltpu.roll(r0, 64, 1))
            high = jnp.where(c == 0, pltpu.roll(r1, 64, 1), r1)
            chosen[j : j + 1, :] = jnp.where(lane < 64, low, high)

    sub = lax.broadcasted_iota(jnp.int32, (OWN, 128), 0)
    first_block = (x * NZ + z) * NY * NC
    held = [(0, OWN, y, c, 0), (OWN, OWN, y, other, 0)]
    for place, core in ((2 * OWN, c), (3 * OWN, other)):
        held += [(place, HALF, at_y(-1), core, 0), (place + HALF, HALF, at_y(1), core, HALF)]
    parts = [(place, lists, (first_block + hy * NC + hc) * OWN + first) for place, lists, hy, hc, first in held]

    def group_logits(r):
        group = jnp.where(c == 0, at_z(GROUPS[0][r]), at_z(GROUPS[1][r]))
        start = pl.multiple_of(group * GROUP, GROUP)
        rows = q[pl.ds(group * NX, NX)].reshape(GROUP, D)
        block = lax.dot_general(
            table[...], rows, (((1,), (1,)), ((), ())), preferred_element_type=jnp.float32
        )
        logits[:, pl.ds(start, GROUP)] = block
        peak = jnp.max(block, axis=0, keepdims=True)
        mass = jnp.sum(jnp.exp(block - peak), axis=0, keepdims=True)
        local_norm = peak + jnp.log(mass)
        for h in range(2):
            tile = group * 2 + h
            norm[pl.ds(tile, 1), :] = local_norm[:, h * 128 : h * 128 + 128]
            ids = chosen[pl.ds(tile, 1), :]
            found = jnp.zeros((1, 128), jnp.float32)
            for place, lists, first in parts:
                values = block[place : place + lists, h * 128 : h * 128 + 128]
                found = found + jnp.sum(jnp.where(sub[:lists] == ids - first, values, 0.0), axis=0, keepdims=True)
            hit[pl.ds(tile, 1), :] = found

    table_sends = []
    table_routes = [
        (0, 2 * OWN, HALF, {"y": at_y(1)}),
        (1, 2 * OWN + HALF, HALF, {"y": at_y(-1)}),
        (0, 3 * OWN, HALF, {"y": at_y(1), "c": other}),
        (1, 3 * OWN + HALF, HALF, {"y": at_y(-1), "c": other}),
        (0, OWN, OWN, partner),
    ]

    def share_table():
        local[PIECES].wait()
        table[:OWN, :] = cent[...].astype(jnp.bfloat16)
        for k, (half, place, rows, where) in enumerate(table_routes):
            source, target = table.at[pl.ds(half * HALF, rows)], table.at[pl.ds(place, rows)]
            table_sends.append(remote(source, target, t_send.at[k], t_recv.at[k], where))

    for core in range(NC):
        send, _ = carriers[core]

        @pl.when(c == core)
        def _(send=send, core=core):
            for p in range(PIECES):
                send(0, 0, p, STARTS[core][p])

    share_table()
    local[PIECES + 1].wait()
    for r in range(8):
        move(r)
        if r == 0:
            choose()
            for k, (_, place, rows, _) in enumerate(table_routes):
                arrived(table.at[pl.ds(place, rows)], t_recv.at[k])
        group_logits(r)
    for _, count in carriers:
        assert count[0] == SENDS

    me1 = lax.div(y, 2) * NX + x

    def exchange1(slots, send, recv):
        for k, (dx, dy) in enumerate(group1):
            remote(slots.at[me1], slots.at[me1], send.at[k], recv.at[me1], {"x": at_x(dx), "y": at_y(dy)})

    def wait1(slots, send, recv):
        for dx, dy in group1:
            place = lax.div(at_y(dy), 2) * NX + at_x(dx)
            arrived(slots.at[place], recv.at[place])

    def exchange2(slots, send, recv):
        for k, dz in enumerate(group2):
            remote(slots.at[z], slots.at[z], send.at[k], recv.at[z], {"z": at_z(dz)})

    def wait2(slots, send, recv):
        for dz in group2:
            arrived(slots.at[at_z(dz)], recv.at[at_z(dz)])

    def summed(slots):
        total = slots[0]
        for k in range(1, 8):
            total = total + slots[k]
        return total

    stat1[me1] = norm[...]
    exchange1(stat1, s1_send, s1_recv)
    hit1[me1] = hit[...]
    exchange1(hit1, h1_send, h1_recv)
    wait1(stat1, s1_send, s1_recv)
    stat2[z] = log_sum_exp([stat1[k] for k in range(8)])
    exchange2(stat2, s2_send, s2_recv)
    wait2(stat2, s2_send, s2_recv)
    norm[...] = log_sum_exp([stat2[k] for k in range(8)])

    wait1(hit1, h1_send, h1_recv)
    here = lax.rem(lax.div(chosen[...], OWN * NY * NC), NZ) == z
    missed = jnp.where(here, norm[...] - summed(hit1), 0.0)
    loss2[z] = missed[:8] + missed[8:]
    exchange2(loss2, h2_send, h2_recv)

    def make_weights(some):
        def tile_weights(j, carry):
            start = pl.multiple_of(j * 128, 128)
            log_norm = norm[pl.ds(j, 1), :]
            ids = chosen[pl.ds(j, 1), :]
            for place, lists, first in some:
                soft = jnp.exp(logits[pl.ds(place, lists), pl.ds(start, 128)] - log_norm)
                soft = jnp.where(sub[:lists] == ids - first, soft - 1.0, soft)
                weights[pl.ds(place, lists), pl.ds(start, 128)] = soft.astype(jnp.bfloat16)
            return carry

        lax.fori_loop(0, TILES, tile_weights, 0)

    def pair_gradient(first, n):
        part[n, first * OWN : (first + 2) * OWN, :] = jnp.dot(
            weights[first * OWN : (first + 2) * OWN, :],
            q[:, :, :, n * WIDTH : (n + 1) * WIDTH].reshape(DEV_ROWS, WIDTH),
            preferred_element_type=jnp.float32,
        )

    to_partner, to_owner, outs = [], [], []

    def hand_over(n, slot):
        lists = part.at[n, pl.ds((1 + 2 * slot) * OWN, OWN)]
        to_partner.append(remote(lists, from_partner.at[n, slot], d_send.at[n, slot], d_recv.at[n, slot], partner))

    def give_back(n):
        arrived(from_partner.at[n, 1], d_recv.at[n, 1])
        y_out[n] = part[n, 2 * OWN : 3 * OWN, :] + from_partner[n, 1]
        for h, k in enumerate((-1, 1)):
            source, target = y_out.at[n, pl.ds(h * HALF, HALF)], y_in.at[n, pl.ds(h * HALF, HALF)]
            to_owner.append(remote(source, target, y_send.at[n, h], y_recv.at[n, h], {"y": at_y(k)}))

    make_weights(parts[2:])
    for n in range(PARTS):
        pair_gradient(2, n)
        hand_over(n, 1)
    make_weights(parts[:2])
    for n in range(PARTS):
        give_back(n)
    wait2(loss2, h2_send, h2_recv)
    loss[0] = summed(loss2)
    loss_across = remote(loss.at[0], loss.at[1], l_send.at[0], l_recv.at[0], partner)
    for n in range(PARTS):
        pair_gradient(0, n)
        hand_over(n, 0)
    loss_across.wait()
    loss[2] = loss[0] + loss[1]
    loss_back = remote(loss.at[2], loss.at[3], l_send.at[1], l_recv.at[1], {"y": at_y(1)})
    for n in range(PARTS):
        arrived(from_partner.at[n, 0], d_recv.at[n, 0])
        for h in range(2):
            arrived(y_in.at[n, pl.ds(h * HALF, HALF)], y_recv.at[n, h])
        grad[n] = part[n, :OWN, :] + from_partner[n, 0] + y_in[n]
        out = pltpu.make_async_copy(grad.at[n], grad_hbm.at[:, pl.ds(n * WIDTH, WIDTH)], g_sem.at[n])
        out.start()
        outs.append(out)
    loss_back.wait()
    loss_ref[...] = jnp.sum(loss[2] + loss[3], keepdims=True) * (1.0 / ROWS)

    for k in range(SENDS):
        arrived(q.at[0, 0], q_send.at[k])
    for slots, send in ((stat1, s1_send), (hit1, h1_send), (stat2, s2_send), (loss2, h2_send)):
        for k in range(7):
            arrived(slots.at[0], send.at[k])
    for copy in table_sends + to_partner + to_owner:
        copy.wait_send()
    for copy in outs:
        copy.wait()


def shards(query_emb, positive_list, centroids, first_moment, second_moment):
    f32, bf16, i32, dma = jnp.float32, jnp.bfloat16, jnp.int32, pltpu.SemaphoreType.DMA
    vmem, hbm = pl.BlockSpec(memory_space=pltpu.VMEM), pl.BlockSpec(memory_space=pl.ANY)
    gradient, loss = pl.pallas_call(
        kernel,
        name="step",
        out_shape=(jax.ShapeDtypeStruct((OWN, D), f32), jax.ShapeDtypeStruct((1, 1), f32)),
        in_specs=[hbm, hbm, hbm],
        out_specs=(hbm, vmem),
        scratch_shapes=[
            pltpu.VMEM((BLOCKS, PIECES, PIECE, D), bf16),
            pltpu.VMEM((ROWS // 128, 128), i32),
            pltpu.VMEM((OWN, D), f32),
            pltpu.VMEM((TILES, 128), i32),
            pltpu.VMEM((HELD, D), bf16),
            pltpu.VMEM((HELD, DEV_ROWS), f32),
            pltpu.VMEM((HELD, DEV_ROWS), bf16),
            pltpu.VMEM((TILES, 128), f32),
            pltpu.VMEM((TILES, 128), f32),
            pltpu.VMEM((8, TILES, 128), f32),
            pltpu.VMEM((8, TILES, 128), f32),
            pltpu.VMEM((8, TILES, 128), f32),
            pltpu.VMEM((8, 8, 128), f32),
            pltpu.VMEM((4, 8, 128), f32),
            pltpu.VMEM((PARTS, HELD, WIDTH), f32),
            pltpu.VMEM((PARTS, 2, OWN, WIDTH), f32),
            pltpu.VMEM((PARTS, OWN, WIDTH), f32),
            pltpu.VMEM((PARTS, OWN, WIDTH), f32),
            pltpu.VMEM((PARTS, OWN, WIDTH), f32),
            dma((PIECES + 2,)), dma((SENDS,)), dma((BLOCKS * PIECES,)), dma((5,)), dma((5,)),
            dma((7,)), dma((8,)), dma((7,)), dma((8,)), dma((7,)), dma((8,)), dma((7,)), dma((8,)), dma((2,)), dma((2,)),
            dma((PARTS, 2)), dma((PARTS, 2)), dma((PARTS, 2)), dma((PARTS, 2)), dma((PARTS,)),
        ],
        compiler_params=pltpu.CompilerParams(collective_id=0, has_side_effects=True, vmem_limit_bytes=65800000),
    )(query_emb, positive_list.reshape(ROWS // 128, 128), centroids)
    return (*adam_update(centroids, first_moment, second_moment, gradient), loss[0, 0])


def solution(mesh):
    split = Mesh(mesh.devices.reshape(NX, NZ, NY, NC), AXES)
    placed = (P(DP, None), P(), P(DP_MP, None), P(DP_MP, None), P(DP_MP, None))
    return jax.shard_map(
        shards,
        mesh=split,
        in_specs=placed,
        out_specs=(P(DP_MP, None), P(DP_MP, None), P(DP_MP, None), P()),
        check_vma=False,
    )
```
